128 devices in a mesh: gx: 8 (over x, y_hi), gy: 16 (over y_lo, z, core).
Axes of the slice: x: 4, y: 4 (y_hi: 2, y_lo: 2; y = y_hi * 2 + y_lo), z: 4, core: 2. Of those that a mesh axis runs over, the one named last changes fastest.
Arguments:
- value_field: float32 [4, 48, 96, 1536], P(None, 'gx', 'gy'), may hold values from -16 to 17
- target_mask: int32 [4, 48, 96, 1536], P(None, 'gx', 'gy'), may hold values 0 or 1
- obstacle_mask: int32 [4, 48, 96, 1536], P(None, 'gx', 'gy'), may hold values 0 or 1
- drift_gains: float32 [5], replicated, may hold values from 0.5 to 2
- control_costs: float32 [5], replicated, may hold values from 0.25 to 1
Outputs:
- reach_value: float32 [4, 48, 96, 1536], P(None, 'gx', 'gy')
- time_steps: float32 [3], replicated
The draws below stay inside these ranges and needn't reach their ends.
All inputs are finite; a program needn't handle non-finite values. No bound on the sum of `target_mask` or of `obstacle_mask` on one device may be relied on, other than what follows from the above.
Results may differ from the reference program's by a relative error of at most 0.0003.
Values sent between devices are 32-bit elements; how exact they have to be, the bound alone decides.
A program may use at most 128 MiB of HBM per device.

```python
import math
import jax
import jax.numpy as jnp
from jax import lax

PLANES = 4
N3 = 32
N4 = 48
GRID = 96
STEPS = 3
NA = 48
NB = 96


def draw_value_field(key, part):
    base_key = jax.random.fold_in(key, 11)
    rough_key, row_key, col_key = jax.random.split(base_key, 3)
    grid_shape = (PLANES, NA, NB, N3 * N4)
    rough_part = jnp.clip(jax.random.normal(rough_key, grid_shape, jnp.float32), -4.0, 4.0)
    row_scale = jnp.exp(jax.random.uniform(row_key, (NA,), jnp.float32, -math.log(2.0), math.log(2.0)))
    col_scale = jnp.exp(jax.random.uniform(col_key, (NB,), jnp.float32, -math.log(2.0), math.log(2.0)))
    return rough_part * row_scale[None, :, None, None] * col_scale[None, None, :, None]


def with_ends(values, own_key, smallest, largest):
    place = [jax.random.randint(jax.random.fold_in(own_key, axis), (), 0, length) for axis, length in enumerate(values.shape)]
    main_axis = values.shape.index(max(values.shape))
    neighbour = place[:main_axis] + [(place[main_axis] + 1) % values.shape[main_axis]] + place[main_axis + 1:]
    return values.at[tuple(place)].set(smallest).at[tuple(neighbour)].set(largest)


def setup_inputs(seed: int = 0) -> dict:
    splits = jax.random.split(jax.random.key(seed), 6)
    return {
        "value_field": draw_value_field(jax.random.fold_in(splits[5], 71), 0),
        "target_mask": with_ends((jax.random.randint(splits[1], (PLANES, NA, NB, N3 * N4), 0, 4) < 1).astype(jnp.int32), jax.random.fold_in(splits[1], 1), 0, 1),
        "obstacle_mask": with_ends((jax.random.randint(splits[2], (PLANES, NA, NB, N3 * N4), 0, 5) < 1).astype(jnp.int32), jax.random.fold_in(splits[2], 1), 0, 1),
        "drift_gains": jnp.clip(jnp.exp(jax.random.uniform(splits[3], (5,), jnp.float32, math.log(0.5), math.log(2.0))), 0.5, 2.0),
        "control_costs": jnp.clip(jnp.exp(jax.random.uniform(splits[4], (5,), jnp.float32, math.log(0.25), math.log(1.0))), 0.25, 1.0),
    }


courant = 0.5
weno_eps = 1e-6


def weno_side(diff_one, diff_two, diff_three, diff_four, diff_five):
    stencil_one = diff_one / 3.0 - 7.0 * diff_two / 6.0 + 11.0 * diff_three / 6.0
    stencil_two = -diff_two / 6.0 + 5.0 * diff_three / 6.0 + diff_four / 3.0
    stencil_three = diff_three / 3.0 + 5.0 * diff_four / 6.0 - diff_five / 6.0
    smooth_one = 13.0 / 12.0 * (diff_one - 2.0 * diff_two + diff_three) ** 2 + 0.25 * (diff_one - 4.0 * diff_two + 3.0 * diff_three) ** 2
    smooth_two = 13.0 / 12.0 * (diff_two - 2.0 * diff_three + diff_four) ** 2 + 0.25 * (diff_two - diff_four) ** 2
    smooth_three = 13.0 / 12.0 * (diff_three - 2.0 * diff_four + diff_five) ** 2 + 0.25 * (3.0 * diff_three - 4.0 * diff_four + diff_five) ** 2
    weight_one = 0.1 / (weno_eps + smooth_one) ** 2
    weight_two = 0.6 / (weno_eps + smooth_two) ** 2
    weight_three = 0.3 / (weno_eps + smooth_three) ** 2
    return (weight_one * stencil_one + weight_two * stencil_two + weight_three * stencil_three) / (weight_one + weight_two + weight_three)


def axis_slopes(shifted, spacing):
    differences = [shifted[offset + 1] - shifted[offset] for offset in range(6)]
    minus_slope = weno_side(differences[0], differences[1], differences[2], differences[3], differences[4]) / spacing
    plus_slope = weno_side(differences[5], differences[4], differences[3], differences[2], differences[1]) / spacing
    return minus_slope, plus_slope


def merged_shifts(interior, stride, position, extent):
    upward = []
    current = interior
    for offset in range(1, 4):
        current = jnp.where(position + offset <= extent - 1, jnp.roll(interior, -offset * stride, axis=-1), current)
        upward.append(current)
    downward = []
    current = interior
    for offset in range(1, 4):
        current = jnp.where(position - offset >= 0, jnp.roll(interior, offset * stride, axis=-1), current)
        downward.append(current)
    return [downward[2], downward[1], downward[0], interior, upward[0], upward[1], upward[2]]


def drift_field(first_pos, heading_one, heading_two, third_pos, fourth_pos, drift_gains):
    return [drift_gains[0] * (jnp.cos(heading_one) - 0.5 * jnp.cos(heading_two) + third_pos),
            drift_gains[1] * (fourth_pos - 0.3 * first_pos),
            drift_gains[2] * (third_pos + 0.5 * jnp.sin(heading_one)),
            drift_gains[3] * (jnp.sin(heading_two) - first_pos),
            drift_gains[4] * (jnp.cos(heading_one) * jnp.sin(heading_two) - fourth_pos)]


def local_bounds(drift_terms, slopes, control_costs, spacing_list):
    peaks = []
    for axis_number in range(5):
        scale = control_costs[axis_number] * spacing_list[axis_number]
        minus_peak = jnp.max(jnp.abs(drift_terms[axis_number] - scale * slopes[axis_number][0]))
        plus_peak = jnp.max(jnp.abs(drift_terms[axis_number] - scale * slopes[axis_number][1]))
        peaks.append(jnp.maximum(minus_peak, plus_peak))
    return jnp.stack(peaks)


def advance(interior, slopes, drift_terms, bounds, time_step, control_costs, spacing_list, target_plane, obstacle_plane):
    hamiltonian = jnp.zeros_like(interior)
    for axis_number in range(5):
        minus_slope, plus_slope = slopes[axis_number]
        middle = 0.5 * (minus_slope + plus_slope)
        hamiltonian = hamiltonian + drift_terms[axis_number] * middle - 0.5 * control_costs[axis_number] * spacing_list[axis_number] * middle * middle
        hamiltonian = hamiltonian - bounds[axis_number] * 0.5 * (plus_slope - minus_slope)
    advanced = interior - time_step * hamiltonian
    advanced = jnp.where(target_plane == 1, jnp.minimum(advanced, -0.5), advanced)
    return jnp.where(obstacle_plane == 1, jnp.maximum(advanced, 0.5), advanced)


def plane_state(padded, plane_index, drift_gains, spacing_list):
    center = lax.dynamic_index_in_dim(padded, plane_index, 0, keepdims=False)
    interior = center[3:-3, 3:-3]
    neighbours = [lax.dynamic_index_in_dim(padded, jnp.clip(plane_index + offset - 3, 0, PLANES - 1).astype(jnp.int32), 0, keepdims=False)[3:-3, 3:-3] for offset in range(7)]
    row_shifts = [center[offset:offset + NA, 3:-3] for offset in range(7)]
    col_shifts = [center[3:-3, offset:offset + NB] for offset in range(7)]
    lane_index = jnp.arange(N3 * N4, dtype=jnp.int32)
    slopes = [axis_slopes(neighbours, spacing_list[0]),
              axis_slopes(row_shifts, spacing_list[1]),
              axis_slopes(col_shifts, spacing_list[2]),
              axis_slopes(merged_shifts(interior, N4, lane_index // N4, N3), spacing_list[3]),
              axis_slopes(merged_shifts(interior, 1, lane_index % N4, N4), spacing_list[4])]
    first_pos = (plane_index.astype(jnp.float32) - PLANES / 2 + 0.5) * (2.0 / GRID)
    heading_one = ((2.0 * math.pi / NA) * jnp.arange(NA, dtype=jnp.float32)).reshape(NA, 1, 1)
    heading_two = ((2.0 * math.pi / NB) * jnp.arange(NB, dtype=jnp.float32)).reshape(1, NB, 1)
    third_pos = (((lane_index // N4).astype(jnp.float32) - N3 / 2 + 0.5) * (2.0 / GRID)).reshape(1, 1, -1)
    fourth_pos = (((lane_index % N4).astype(jnp.float32) - N4 / 2 + 0.5) * (2.0 / GRID)).reshape(1, 1, -1)
    drift_terms = drift_field(first_pos, heading_one, heading_two, third_pos, fourth_pos, drift_gains)
    return interior, slopes, drift_terms


def reference(value_field, target_mask, obstacle_mask, drift_gains, control_costs):
    spacing_list = [2.0 / GRID, 2.0 * math.pi / NA, 2.0 * math.pi / NB, 2.0 / GRID, 2.0 / GRID]
    spacing_array = jnp.array(spacing_list, dtype=jnp.float32)
    plane_ids = jnp.arange(PLANES, dtype=jnp.int32)
    value_now = value_field
    step_sizes = []
    for section_number in range(STEPS):
        padded = jnp.pad(value_now, ((0, 0), (3, 3), (3, 3), (0, 0)), mode="wrap")

        def bound_plane(plane_index):
            interior, slopes, drift_terms = plane_state(padded, plane_index, drift_gains, spacing_list)
            return local_bounds(drift_terms, slopes, control_costs, spacing_list)

        bounds = jnp.max(lax.map(bound_plane, plane_ids), axis=0)
        time_step = courant / (jnp.sum(bounds / spacing_array) + 1e-6)

        def move_plane(items):
            plane_index, target_plane, obstacle_plane = items
            interior, slopes, drift_terms = plane_state(padded, plane_index, drift_gains, spacing_list)
            return advance(interior, slopes, drift_terms, bounds, time_step, control_costs, spacing_list, target_plane, obstacle_plane)

        value_now = lax.map(move_plane, (plane_ids, target_mask, obstacle_mask))
        step_sizes.append(time_step)
    return value_now, jnp.stack(step_sizes)
```

```python
import functools
import math

import jax
import jax.numpy as jnp
from jax import lax
from jax.experimental import pallas as pl
from jax.experimental.pallas import tpu as pltpu
from jax.sharding import PartitionSpec as P

PLANES, N3, N4, GRID, STEPS, NA, NB = 4, 32, 48, 96, 3, 48, 96
SPACING = (2.0 / GRID, 2.0 * math.pi / NA, 2.0 * math.pi / NB, 2.0 / GRID, 2.0 / GRID)
MESH = pl.DeviceIdType.MESH
F32 = jnp.float32
BIG = 3.0e38

ROWS_A, COLS_B, CHUNKS = 12, 6, 6
CELL = PLANES * CHUNKS
LINE = COLS_B * CELL
TOTAL = ROWS_A * LINE
GROUPS = 5
PADDED = GROUPS * 384
PITCH = 52
SLOTS = 14
GHOST = 3
EPS = 0.75e-6


def _add(x, y):
    if x is None:
        return y
    if y is None:
        return x
    return x + y


def _sub(x, y):
    if y is None:
        return x
    if x is None:
        return -y
    return x - y


def _mul(x, y):
    if x is None or y is None:
        return None
    return x * y


def chain(values):
    cells = len(values) - 6
    diffs = [
        None if values[i] is values[i + 1] else values[i + 1] - values[i]
        for i in range(cells + 5)
    ]
    curve, twice, lean, weight_x, weight_y, weight_z = {}, {}, {}, {}, {}, {}
    previous = None

    def curve_at(i):
        if i not in curve:
            curve[i] = _sub(diffs[i + 1], diffs[i])
            twice[i] = _add(curve[i], curve[i])
            square = _mul(curve[i], curve[i])
            lean[i] = (square, _mul(square, 1.5))
        return curve[i]

    def smooth_at(i):
        if i not in weight_x:
            now, last = curve_at(i), curve_at(i - 1)
            cross = _mul(now, last)
            base = _add(lean[i][0], lean[i - 1][0])
            base = EPS if base is None else base + EPS
            middle = _sub(base, _mul(cross, 2.75))
            x = _add(middle, lean[i][1])
            y = _add(middle, lean[i - 1][1])
            z = _add(middle, _mul(cross, 1.5))
            weight_x[i], weight_y[i], weight_z[i] = x * x, y * y, z * z

    def third_at(i):
        return _sub(_add(curve_at(i + 1), curve_at(i - 1)), twice[i])

    thirds = {}
    for face in range(2, cells + 3):
        for i in (face - 1, face, face + 1):
            smooth_at(i)
        one, two, three = weight_x[face - 1], weight_z[face], weight_y[face + 1]
        w_low, w_mid, w_high = two * three, one * three, one * two
        for i in (face - 1, face):
            if i not in thirds:
                thirds[i] = third_at(i)
        low = _mul(thirds[face - 1], w_low)
        high = _mul(thirds[face], w_high)
        base = ((w_low + w_high) + (w_mid + w_mid)) * 1.5
        now, last = curve[face], curve[face - 1]
        scaled = _mul(diffs[face], 6.0)
        left = right = None
        if face < cells + 2:
            top = _add(low, _mul(high, 1.5))
            left = _add(scaled, _add(last, twice[face]))
            if top is not None:
                left = _sub(left, top * pl.reciprocal(base - w_low, approx=True))
        if face > 2:
            top = _add(_mul(low, 1.5), high)
            right = _sub(scaled, _add(now, twice[face - 1]))
            if top is not None:
                right = _add(right, top * pl.reciprocal(base - w_high, approx=True))
            yield previous, right
        previous = left


def kernel(
    value_hbm, target_hbm, obstacle_hbm, gains, costs,
    out_hbm, steps_out,
    val, hn, d_a, d_b, d_p, wn, hi, lo,
    ghost_al, ghost_ah, ghost_bl, ghost_bh,
    tr, ht, d_3, d_4, side_out, side_in,
    stage_own, stage_other, mask_own, mask_other,
    tab_f1, tab_f2, tab_sa, tab_ab, tab_x3, tab_l3, tab_l4,
    ar_src, ar_buf,
    local_sem, swap_s, swap_r, halo_s, halo_r, ar_s, ar_r, out_sem, out_s, out_r,
):
    gx, gy = lax.axis_index("gx"), lax.axis_index("gy")
    half = lax.rem(gx, 2)
    other = 1 - half
    partner = (gx + 1 - 2 * half, gy)
    me = gx * 16 + gy

    def remote(src, dst, send, recv, device):
        return pltpu.make_async_remote_copy(
            src_ref=src, dst_ref=dst, send_sem=send, recv_sem=recv,
            device_id=device, device_id_type=MESH,
        )

    def lanes_of(ref, which):
        return ref.at[:, :, :, pl.ds(pl.multiple_of(which * 768, 128), 768)]

    inputs = (value_hbm, target_hbm, obstacle_hbm)
    others = (stage_other, mask_other.at[0], mask_other.at[1])
    owns = (stage_own, mask_own.at[0], mask_own.at[1])
    swaps = [
        remote(lanes_of(inputs[k], other), others[k], swap_s.at[k], swap_r.at[k], partner)
        for k in range(3)
    ]
    locals_ = [
        pltpu.make_async_copy(lanes_of(inputs[k], half), owns[k], local_sem.at[k])
        for k in range(3)
    ]
    swaps[0].start()
    for k in range(3):
        locals_[k].start()

    lane8 = lax.broadcasted_iota(jnp.int32, (8, 128), 1)
    lane8f = lane8.astype(F32)
    odd = (lane8 & 1) == 1

    def splat(scalar):
        return jnp.full((8, 128), scalar, F32)

    fscale = [splat(12.0 * gains[i]) / splat(costs[i]) for i in range(5)]
    kk = [costs[i] * (1.0 / (288.0 * SPACING[i])) for i in range(5)]
    half_f = half.astype(F32)
    first_a = (lax.div(gx, 2) * ROWS_A).astype(F32)
    first_b = (gy * COLS_B).astype(F32)
    step_a, step_b = 2.0 * math.pi / NA, 2.0 * math.pi / NB
    cell = 2.0 / GRID

    def split_lane(merged):
        third = jnp.floor((merged + 0.5) * (1.0 / N4))
        return third, merged - third * N4

    for block in range(3):
        row = lax.broadcasted_iota(jnp.int32, (8, 128), 0).astype(F32) + 8.0 * block
        plane = jnp.floor((row + 0.5) * (1.0 / CHUNKS))
        merged = (half_f * CHUNKS + row - plane * CHUNKS) * 128.0 + lane8f
        third, fourth = split_lane(merged)
        x0 = (plane - PLANES / 2 + 0.5) * cell
        x3 = (third - N3 / 2 + 0.5) * cell
        x4 = (fourth - N4 / 2 + 0.5) * cell
        tab_f1[pl.ds(8 * block, 8)] = fscale[1] * (x4 - 0.3 * x0)
        tab_f2[pl.ds(8 * block, 8)] = fscale[2] * x3
    for chunk in range(CHUNKS):
        third, _ = split_lane((half_f * CHUNKS + chunk) * 128.0 + lane8f)
        tab_x3[pl.ds(8 * chunk, 8)] = fscale[0] * ((third - N3 / 2 + 0.5) * cell)

    def table_row(i, carry):
        angle = step_a * (splat(first_a) + i.astype(F32))
        tab_sa[pl.ds(pl.multiple_of(8 * i, 8), 8)] = fscale[2] * (0.5 * jnp.sin(angle))
        return carry

    lax.fori_loop(0, ROWS_A, table_row, 0)

    def table_ab(i, carry):
        row = lax.broadcasted_iota(jnp.int32, (8, 128), 0).astype(F32) + 8.0 * i.astype(F32)
        a = jnp.floor((row + 0.5) * (1.0 / COLS_B))
        b = row - a * COLS_B
        tab_ab[pl.ds(pl.multiple_of(8 * i, 8), 8)] = fscale[0] * (
            jnp.cos(step_a * (first_a + a)) - 0.5 * jnp.cos(step_b * (first_b + b))
        )
        return carry

    lax.fori_loop(0, 9, table_ab, 0)

    def table_lane(g, carry):
        spot = lane8f + 128.0 * g.astype(F32)
        pair = jnp.floor((spot + 0.5) * 0.125)
        plane = jnp.floor((spot - pair * 8.0 + 0.5) * 0.5)
        a = jnp.floor((pair + 0.5) * (1.0 / COLS_B))
        b = pair - a * COLS_B
        sin_b = jnp.sin(step_b * (first_b + b))
        x0 = (plane - PLANES / 2 + 0.5) * cell
        keep = spot < 576.0
        where = pl.ds(pl.multiple_of(8 * g, 8), 8)
        tab_l3[where] = jnp.where(keep, fscale[3] * (sin_b - x0), 0.0)
        tab_l4[where] = jnp.where(keep, fscale[4] * (jnp.cos(step_a * (first_a + a)) * sin_b), 0.0)
        return carry

    lax.fori_loop(0, GROUPS, table_lane, 0)
    for i in range(TOTAL // 8, PADDED // 8):
        val[pl.ds(8 * i, 8)] = jnp.zeros((8, 128), F32)

    def spread(stage, target_rows, convert=None):
        def body(a, carry):
            for p in range(PLANES):
                for c in range(CHUNKS):
                    tile = stage[p, a, :, pl.ds(128 * c, 128)]
                    start = (target_rows + a) * LINE + p * CHUNKS + c
                    if convert is None:
                        val[pl.ds(start, COLS_B, stride=CELL)] = tile
                    else:
                        ref, bound, free = convert
                        ref[pl.ds(start, COLS_B, stride=CELL)] = jnp.where(tile == 1, bound, free)
            return carry

        lax.fori_loop(0, 6, body, 0)

    locals_[0].wait()
    spread(stage_own, half * 6)
    swaps[0].wait_recv()
    spread(stage_other, other * 6)

    row_before = (lax.rem(gx + 6, 8), gy)
    row_after = (lax.rem(gx + 2, 8), gy)
    col_before = (gx, lax.rem(gy + 15, 16))
    col_after = (gx, lax.rem(gy + 1, 16))

    def whole(ref, k):
        return remote(ref, ref, halo_s.at[k], halo_r.at[k], partner)

    halo_refs = (ghost_al, ghost_ah, ghost_bl, ghost_bh, side_in)

    def start_side():
        remote(side_out, side_in, halo_s.at[4], halo_r.at[4], partner).start()

    def start_halos():
        for a in range(ROWS_A):
            remote(
                val.at[pl.ds(a * LINE + 72, 72)], ghost_bl.at[pl.ds(a * 72, 72)],
                halo_s.at[2], halo_r.at[2], col_after,
            ).start()
            remote(
                val.at[pl.ds(a * LINE, 72)], ghost_bh.at[pl.ds(a * 72, 72)],
                halo_s.at[3], halo_r.at[3], col_before,
            ).start()
        remote(
            val.at[pl.ds((ROWS_A - 3) * LINE, 3 * LINE)], ghost_al,
            halo_s.at[0], halo_r.at[0], row_after,
        ).start()
        remote(
            val.at[pl.ds(0, 3 * LINE)], ghost_ah,
            halo_s.at[1], halo_r.at[1], row_before,
        ).start()

    def tr_row(g, slot):
        return g * (SLOTS * PITCH) + slot * PITCH

    def to_transposed():
        def body(g, carry):
            for r in range(3):
                block = val[pl.ds(g * 384 + r, 128, stride=3)].T
                for k in range(16):
                    merged = r * 128 + 8 * k
                    row = tr_row(g, GHOST + merged // N4) + merged % N4
                    tr[pl.ds(row, 8)] = block[8 * k:8 * k + 8]
            return carry

        lax.fori_loop(0, GROUPS, body, 0)

    is_low = half == 0
    turn = jnp.where(is_low, 127, 1)
    mine = jnp.where(is_low, lane8 & 1, 1 - (lane8 & 1)) == 0
    send_slot = jnp.where(is_low, GHOST + 5, GHOST)

    def pack_side():
        def body(k, carry):
            for s in range(3):
                for q in range(6):
                    one = tr[pl.ds(tr_row(2 * k, send_slot + s) + 8 * q, 8)]
                    two = tr[pl.ds(tr_row(jnp.minimum(2 * k + 1, 4), send_slot + s) + 8 * q, 8)]
                    side_out[pl.ds(k * 144 + s * 48 + 8 * q, 8)] = jnp.where(
                        mine, pltpu.roll(one, turn, 1), two
                    )
            return carry

        lax.fori_loop(0, 3, body, 0)

    def merge_side():
        def body(g, carry):
            pack = lax.div(g, 2)
            second = lax.rem(g, 2) == 1
            back = jnp.where(is_low, 1, 127)
            for s in range(3):
                for q in range(6):
                    at = 8 * q
                    got = side_in[pl.ds(pack * 144 + s * 48 + at, 8)]
                    got = jnp.where(second, pltpu.roll(got, back, 1), got)
                    top = tr[pl.ds(tr_row(g, GHOST + 7) + at, 8)]
                    bottom = tr[pl.ds(tr_row(g, GHOST) + at, 8)]
                    up = pltpu.roll(tr[pl.ds(tr_row(g, GHOST + s) + at, 8)], 127, 1)
                    down = pltpu.roll(tr[pl.ds(tr_row(g, GHOST + 5 + s) + at, 8)], 1, 1)
                    tr[pl.ds(tr_row(g, GHOST + 8 + s) + at, 8)] = jnp.where(
                        odd, jnp.where(is_low, got, top), up
                    )
                    tr[pl.ds(tr_row(g, s) + at, 8)] = jnp.where(
                        odd, down, jnp.where(is_low, bottom, got)
                    )
            return carry

        lax.fori_loop(0, GROUPS, body, 0)

    def cell_out(left, right, flow, square, factor, peak):
        total = left + right
        gap = right - left
        rest = flow - total
        peak = jnp.maximum(peak, jnp.abs(rest) + jnp.abs(gap))
        return gap, (square - rest * rest) * factor, peak

    zero = jnp.zeros((8, 128), F32)

    def along_planes():
        def body(n, peak):
            q, c = lax.div(n, CHUNKS), lax.rem(n, CHUNKS)
            start = q * (8 * CELL) + c
            rows = [pl.ds(start + p * CHUNKS, 8, stride=CELL) for p in range(PLANES)]
            got = [val[rows[p]] for p in range(PLANES)]
            flow = tab_ab[pl.ds(pl.multiple_of(8 * q, 8), 8)] + tab_x3[
                pl.ds(pl.multiple_of(8 * c, 8), 8)
            ]
            square = flow * flow
            line = [got[0]] * 3 + got + [got[3]] * 3
            for p, (left, right) in enumerate(chain(line)):
                left = zero if left is None else left
                right = zero if right is None else right
                gap, part, peak = cell_out(left, right, flow, square, kk[0], peak)
                d_p[rows[p]] = gap
                hn[rows[p]] = part
            return peak

        return lax.fori_loop(0, 9 * CHUNKS, body, zero)

    def along_rows():
        def body(n, peak):
            at = pl.multiple_of(8 * n, 8)
            line = (
                [ghost_al[pl.ds(i * LINE + at, 8)] for i in range(3)]
                + [val[pl.ds(a * LINE + at, 8)] for a in range(ROWS_A)]
                + [ghost_ah[pl.ds(i * LINE + at, 8)] for i in range(3)]
            )
            flow = tab_f1[pl.ds(pl.multiple_of(8 * lax.rem(n, 3), 8), 8)]
            square = flow * flow
            for a, (left, right) in enumerate(chain(line)):
                gap, part, peak = cell_out(left, right, flow, square, kk[1], peak)
                where = pl.ds(a * LINE + at, 8)
                d_a[where] = gap
                hn[where] += part
            return peak

        return lax.fori_loop(0, LINE // 8, body, zero)

    def along_cols():
        def body(n, peak):
            a, j = lax.div(n, 3), lax.rem(n, 3)
            ghost = pl.multiple_of(a * 72 + 8 * j, 8)
            at = pl.multiple_of(a * LINE + 8 * j, 8)
            line = (
                [ghost_bl[pl.ds(ghost + i * CELL, 8)] for i in range(3)]
                + [val[pl.ds(at + b * CELL, 8)] for b in range(COLS_B)]
                + [ghost_bh[pl.ds(ghost + i * CELL, 8)] for i in range(3)]
            )
            flow = tab_f2[pl.ds(pl.multiple_of(8 * j, 8), 8)] + tab_sa[
                pl.ds(pl.multiple_of(8 * a, 8), 8)
            ]
            square = flow * flow
            for b, (left, right) in enumerate(chain(line)):
                gap, part, peak = cell_out(left, right, flow, square, kk[2], peak)
                where = pl.ds(at + b * CELL, 8)
                d_b[where] = gap
                hn[where] += part
            return peak

        return lax.fori_loop(0, 3 * ROWS_A, body, zero)

    def along_third():
        def body(n, peak):
            g, q = lax.div(n, 6), lax.rem(n, 6)
            line = [tr[pl.ds(tr_row(g, s) + 8 * q, 8)] for s in range(SLOTS)]
            flow = tab_l3[pl.ds(pl.multiple_of(8 * g, 8), 8)]
            square = flow * flow
            for s, (left, right) in enumerate(chain(line)):
                gap, part, peak = cell_out(left, right, flow, square, kk[3], peak)
                where = pl.ds((g * 8 + s) * PITCH + 8 * q, 8)
                d_3[where] = gap
                ht[where] += part
            return peak

        return lax.fori_loop(0, GROUPS * 6, body, zero)

    slope4 = fscale[4] * cell

    def along_fourth():
        def body(n, peak):
            g, seg = lax.div(n, 4), lax.rem(n, 4)
            first = seg * 12
            line = []
            for i in range(-3, 15):
                at = first + i
                if i < 0:
                    at = jnp.maximum(at, 0)
                if i > 11:
                    at = jnp.minimum(at, N4 - 1)
                line.append(tr[pl.ds(tr_row(g, GHOST) + at, 8, stride=PITCH)])
            table = tab_l4[pl.ds(pl.multiple_of(8 * g, 8), 8)]
            base = table - slope4 * (first.astype(F32) - (N4 / 2 - 0.5))
            for i, (left, right) in enumerate(chain(line)):
                flow = base - slope4 * float(i)
                gap, part, peak = cell_out(left, right, flow, flow * flow, kk[4], peak)
                where = pl.ds(g * 8 * PITCH + first + i, 8, stride=PITCH)
                d_4[where] = gap
                ht[where] = part
            return peak

        return lax.fori_loop(0, GROUPS * 4, body, zero)

    def speeds(step, peaks):
        row = jnp.zeros((1, 128), F32)
        lane = lax.broadcasted_iota(jnp.int32, (1, 128), 1)
        for i, peak in enumerate(peaks):
            row = jnp.where(lane == i, jnp.max(peak), row)
        ar_src[step] = row
        ar_buf[step, me] = row

        def send(k, carry):
            to = lax.rem(me + k, 128)
            remote(
                ar_src.at[step], ar_buf.at[step, me], ar_s.at[step], ar_r.at[step],
                (lax.div(to, 16), lax.rem(to, 16)),
            ).start()
            return carry

        lax.fori_loop(1, 128, send, 0)

    def all_speeds(step):
        every = ar_buf.at[step, pl.ds(0, 127)]
        whole_row = remote(every, every, ar_s.at[step], ar_r.at[step], partner)
        whole_row.wait_recv()
        best = jnp.max(ar_buf[step], axis=0)
        whole_row.wait_send()
        speed = []
        for i in range(5):
            lane_max = jnp.broadcast_to(best[:, i:i + 1], (8, 128))
            speed.append(lane_max * (costs[i] * (1.0 / 12.0)))
        summed = zero
        for i in range(5):
            summed = summed + speed[i] / SPACING[i]
        time_step = 0.5 / (summed + 1e-6)
        steps_out[step] = time_step[0, 0]
        return time_step, [
            time_step * speed[i] * (1.0 / (12.0 * SPACING[i])) for i in range(5)
        ]

    def from_transposed(dt, coef):
        def body(g, carry):
            for r in range(3):
                parts = []
                for k in range(16):
                    merged = r * 128 + 8 * k
                    row = (g * 8 + merged // N4) * PITCH + merged % N4
                    where = pl.ds(row, 8)
                    parts.append(coef[3] * d_3[where] + coef[4] * d_4[where] - dt * ht[where])
                block = jnp.concatenate(parts, axis=0).T
                wn[pl.ds(g * 384 + r, 128, stride=3)] = block
            return carry

        lax.fori_loop(0, GROUPS, body, 0)

    def new_row(at, dt, coef):
        where = pl.ds(at, 8)
        moved = val[where] + wn[where] - dt * hn[where]
        moved = moved + coef[0] * d_p[where] + coef[1] * d_a[where] + coef[2] * d_b[where]
        return jnp.maximum(jnp.minimum(moved, hi[where]), lo[where])

    def update(dt, coef):
        def body(n, carry):
            for i in range(4):
                at = pl.multiple_of(32 * n + 8 * i, 8)
                val[pl.ds(at, 8)] = new_row(at, dt, coef)
            return carry

        lax.fori_loop(0, TOTAL // 32, body, 0)

    def out_copy(stage, a, which):
        return stage.at[:, a], out_hbm.at[:, a, :, pl.ds(pl.multiple_of(which * 768, 128), 768)]

    def last_update(dt, coef):
        def rows(first, stage, launch):
            def body(a, carry):
                for i in range(LINE // 8):
                    at = pl.multiple_of((first + a) * LINE + 8 * i, 8)
                    val[pl.ds(at, 8)] = new_row(at, dt, coef)
                for p in range(PLANES):
                    for c in range(CHUNKS):
                        start = (first + a) * LINE + p * CHUNKS + c
                        stage[p, a, :, pl.ds(128 * c, 128)] = val[
                            pl.ds(start, COLS_B, stride=CELL)
                        ]
                launch(a)
                return carry

            lax.fori_loop(0, 6, body, 0)

        def far(a):
            src, dst = out_copy(stage_other, a, half)
            remote(src, dst, out_s, out_r, partner).start()

        def near(a):
            src, dst = out_copy(stage_own, a, half)
            pltpu.make_async_copy(src, dst, out_sem).start()

        rows(other * 6, stage_other, far)
        rows(half * 6, stage_own, near)
        done = pltpu.make_async_copy(stage_own, lanes_of(out_hbm, half), out_sem)
        done.wait()
        sent = remote(stage_other, lanes_of(out_hbm, other), out_s, out_r, partner)
        sent.wait_send()
        sent.wait_recv()

    for step in range(STEPS):
        to_transposed()
        pack_side()
        start_side()
        start_halos()
        if step == 0:
            swaps[1].start()
            swaps[2].start()
        peak_p = along_planes()
        peak_4 = along_fourth()
        whole(side_in, 4).wait_recv()
        merge_side()
        peak_3 = along_third()
        whole(ghost_bl, 2).wait_recv()
        whole(ghost_bh, 3).wait_recv()
        peak_b = along_cols()
        whole(ghost_al, 0).wait_recv()
        whole(ghost_ah, 1).wait_recv()
        peak_a = along_rows()
        speeds(step, [peak_p, peak_a, peak_b, peak_3, peak_4])
        for k, ref in enumerate(halo_refs):
            whole(ref, k).wait_send()
        if step == 0:
            for k in (1, 2):
                locals_[k].wait()
            spread(owns[1], half * 6, (hi, -0.5, BIG))
            spread(owns[2], half * 6, (lo, 0.5, -BIG))
            for k in (1, 2):
                swaps[k].wait_recv()
            spread(others[1], other * 6, (hi, -0.5, BIG))
            spread(others[2], other * 6, (lo, 0.5, -BIG))
            for k in range(3):
                swaps[k].wait_send()
        dt, coef = all_speeds(step)
        from_transposed(dt, coef)
        if step < STEPS - 1:
            update(dt, coef)
        else:
            last_update(dt, coef)


def solution(mesh):
    def rows(n):
        return pltpu.VMEM((n, 128), F32)

    dma = pltpu.SemaphoreType.DMA
    stage = (PLANES, 6, 6, 768)
    trans = GROUPS * 8 * PITCH
    scratch = [
        rows(PADDED), rows(TOTAL), rows(TOTAL), rows(TOTAL), rows(TOTAL), rows(PADDED),
        rows(TOTAL), rows(TOTAL),
        rows(3 * LINE), rows(3 * LINE), rows(ROWS_A * 72), rows(ROWS_A * 72),
        rows(GROUPS * SLOTS * PITCH), rows(trans), rows(trans), rows(trans),
        rows(432), rows(432),
        pltpu.VMEM(stage, F32), pltpu.VMEM(stage, F32),
        pltpu.VMEM((2,) + stage, jnp.int32), pltpu.VMEM((2,) + stage, jnp.int32),
        rows(24), rows(24), rows(8 * ROWS_A), rows(72), rows(8 * CHUNKS),
        rows(8 * GROUPS), rows(8 * GROUPS),
        pltpu.VMEM((STEPS, 1, 128), F32), pltpu.VMEM((STEPS, 128, 1, 128), F32),
        dma((3,)), dma((3,)), dma((3,)), dma((5,)), dma((5,)), dma((STEPS,)), dma((STEPS,)),
        dma(()), dma(()), dma(()),
    ]

    def body(value_field, target_mask, obstacle_mask, drift_gains, control_costs):
        anywhere = pl.BlockSpec(memory_space=pl.ANY)
        scalars = pl.BlockSpec(memory_space=pltpu.SMEM)
        return pl.pallas_call(
            kernel,
            out_shape=(
                jax.ShapeDtypeStruct(value_field.shape, F32),
                jax.ShapeDtypeStruct((STEPS,), F32),
            ),
            in_specs=[anywhere, anywhere, anywhere, scalars, scalars],
            out_specs=(anywhere, scalars),
            scratch_shapes=scratch,
            compiler_params=pltpu.CompilerParams(
                has_side_effects=True, vmem_limit_bytes=56 * 2**20
            ),
        )(value_field, target_mask, obstacle_mask, drift_gains, control_costs)

    grid = P(None, "gx", "gy", None)
    return jax.shard_map(
        body, mesh=mesh, in_specs=(grid, grid, grid, P(), P()), out_specs=(grid, P()),
        check_vma=False,
    )
```

```python
import functools
import math

import jax
import jax.numpy as jnp
from jax import lax
from jax.experimental import pallas as pl
from jax.experimental.pallas import tpu as pltpu
from jax.sharding import PartitionSpec as P

PLANES, N3, N4, GRID, STEPS, NA, NB = 4, 32, 48, 96, 3, 48, 96
SPACING = (2.0 / GRID, 2.0 * math.pi / NA, 2.0 * math.pi / NB, 2.0 / GRID, 2.0 / GRID)
MESH = pl.DeviceIdType.MESH
F32 = jnp.float32
BIG = 3.0e38

ROWS_A, COLS_B, CHUNKS = 12, 6, 6
CELL = PLANES * CHUNKS
LINE = COLS_B * CELL
TOTAL = ROWS_A * LINE
GROUPS = 5
PITCH = 52
SLOTS = 14
GHOST = 3
EPS = 0.75e-6


def _hops(offset):
    dx, dy = offset
    ring = lambda n: min(n, 4 - n)
    return ring(dx // 2) + 2 * (dx % 2) + ring(dy // 2 % 4) + dy // 8


FAR_FIRST = sorted(
    [(dx, dy) for dx in range(8) for dy in range(16) if dx or dy], key=_hops, reverse=True
)
ROUNDS = (((0, 1), (0, 15)), ((0, 2), (0, 14)), ((0, 4), (0, 12)), ((2, 0), (6, 0)), ((4, 0),))


def _add(x, y):
    if x is None:
        return y
    if y is None:
        return x
    return x + y


def _sub(x, y):
    if y is None:
        return x
    if x is None:
        return -y
    return x - y


def _mul(x, y):
    if x is None or y is None:
        return None
    return x * y


def chain(values):
    cells = len(values) - 6
    diffs = [
        None if values[i] is values[i + 1] else values[i + 1] - values[i]
        for i in range(cells + 5)
    ]
    curve, twice, lean, weight_x, weight_y, weight_z = {}, {}, {}, {}, {}, {}
    previous = None

    def curve_at(i):
        if i not in curve:
            curve[i] = _sub(diffs[i + 1], diffs[i])
            twice[i] = _add(curve[i], curve[i])
            square = _mul(curve[i], curve[i])
            lean[i] = (square, _mul(square, 1.5))
        return curve[i]

    def smooth_at(i):
        if i not in weight_x:
            now, last = curve_at(i), curve_at(i - 1)
            cross = _mul(now, last)
            base = _add(lean[i][0], lean[i - 1][0])
            base = EPS if base is None else base + EPS
            middle = _sub(base, _mul(cross, 2.75))
            x = _add(middle, lean[i][1])
            y = _add(middle, lean[i - 1][1])
            z = _add(middle, _mul(cross, 1.5))
            weight_x[i], weight_y[i], weight_z[i] = x * x, y * y, z * z

    def third_at(i):
        return _sub(_add(curve_at(i + 1), curve_at(i - 1)), twice[i])

    thirds = {}
    for face in range(2, cells + 3):
        for i in (face - 1, face, face + 1):
            smooth_at(i)
        one, two, three = weight_x[face - 1], weight_z[face], weight_y[face + 1]
        w_low, w_mid, w_high = two * three, one * three, one * two
        for i in (face - 1, face):
            if i not in thirds:
                thirds[i] = third_at(i)
        low = _mul(thirds[face - 1], w_low)
        high = _mul(thirds[face], w_high)
        base = ((w_low + w_high) + (w_mid + w_mid)) * 1.5
        now, last = curve[face], curve[face - 1]
        scaled = _mul(diffs[face], 6.0)
        left = right = None
        if face < cells + 2:
            top = _add(low, _mul(high, 1.5))
            left = _add(scaled, _add(last, twice[face]))
            if top is not None:
                left = _sub(left, top * pl.reciprocal(base - w_low, approx=True))
        if face > 2:
            top = _add(_mul(low, 1.5), high)
            right = _sub(scaled, _add(now, twice[face - 1]))
            if top is not None:
                right = _add(right, top * pl.reciprocal(base - w_high, approx=True))
            yield previous, right
        previous = left


def kernel(
    value_hbm, target_hbm, obstacle_hbm, gains, costs,
    out_hbm, steps_out,
    val, hn, d_a, d_b, d_p, wn, hi, lo,
    ghost_al, ghost_ah, ghost_bl, ghost_bh,
    tr, ht, d_3, d_4, side_out, side_in,
    mask_t, mask_o,
    tab_f1, tab_f2, tab_sa, tab_ab, tab_x3, tab_l3, tab_l4,
    ar_src, ar_buf,
    met, local_sem, swap_s, swap_r, halo_s, halo_r, ar_s, ar_r, out_sem, out_s, out_r,
):
    gx, gy = lax.axis_index("gx"), lax.axis_index("gy")
    half = lax.rem(gx, 2)
    other = 1 - half
    partner = (gx + 1 - 2 * half, gy)
    me = gx * 16 + gy

    def remote(src, dst, send, recv, device):
        return pltpu.make_async_remote_copy(
            src_ref=src, dst_ref=dst, send_sem=send, recv_sem=recv,
            device_id=device, device_id_type=MESH,
        )

    row_before = (lax.rem(gx + 6, 8), gy)
    row_after = (lax.rem(gx + 2, 8), gy)
    col_before = (gx, lax.rem(gy + 15, 16))
    col_after = (gx, lax.rem(gy + 1, 16))
    barrier = pltpu.get_barrier_semaphore()
    for device in (partner, col_before, col_after, row_before, row_after):
        pl.semaphore_signal(barrier, inc=1, device_id=device, device_id_type=MESH)

    def part_of(ref, which):
        return ref.at[:, pl.ds(pl.multiple_of(which * CELL, 8), CELL)]

    inputs = (value_hbm, target_hbm, obstacle_hbm)
    places = (val, mask_t, mask_o)

    def cells_of(ref, first, count):
        return ref.reshape(TOTAL // CELL, CELL, 128).at[pl.ds(first, count)]

    swaps = [
        remote(
            part_of(inputs[k], other), cells_of(places[k], half * 36, 36),
            swap_s.at[k], swap_r.at[k], partner,
        )
        for k in range(3)
    ]
    locals_ = [
        pltpu.make_async_copy(
            part_of(inputs[k], half), cells_of(places[k], half * 36, 36), local_sem.at[k]
        )
        for k in range(3)
    ]
    for k in range(3):
        locals_[k].start()
    pl.semaphore_wait(barrier, 5)
    swaps[0].start()

    lane8 = lax.broadcasted_iota(jnp.int32, (8, 128), 1)
    lane8f = lane8.astype(F32)
    odd = (lane8 & 1) == 1

    def splat(scalar):
        return jnp.full((8, 128), scalar, F32)

    fscale = [splat(12.0 * gains[i]) / splat(costs[i]) for i in range(5)]
    kk = [costs[i] * (1.0 / (288.0 * SPACING[i])) for i in range(5)]
    half_f = half.astype(F32)
    first_a = (lax.div(gx, 2) * ROWS_A).astype(F32)
    first_b = (gy * COLS_B).astype(F32)
    step_a, step_b = 2.0 * math.pi / NA, 2.0 * math.pi / NB
    cell = 2.0 / GRID

    def split_lane(merged):
        third = jnp.floor((merged + 0.5) * (1.0 / N4))
        return third, merged - third * N4

    for block in range(3):
        row = lax.broadcasted_iota(jnp.int32, (8, 128), 0).astype(F32) + 8.0 * block
        chunk = jnp.floor((row + 0.5) * (1.0 / PLANES))
        plane = row - chunk * PLANES
        merged = (half_f * CHUNKS + chunk) * 128.0 + lane8f
        third, fourth = split_lane(merged)
        x0 = (plane - PLANES / 2 + 0.5) * cell
        x3 = (third - N3 / 2 + 0.5) * cell
        x4 = (fourth - N4 / 2 + 0.5) * cell
        tab_f1[pl.ds(8 * block, 8)] = fscale[1] * (x4 - 0.3 * x0)
        tab_f2[pl.ds(8 * block, 8)] = fscale[2] * x3
    for chunk in range(CHUNKS):
        third, _ = split_lane((half_f * CHUNKS + chunk) * 128.0 + lane8f)
        tab_x3[pl.ds(8 * chunk, 8)] = fscale[0] * ((third - N3 / 2 + 0.5) * cell)

    def table_row(i, carry):
        angle = step_a * (splat(first_a) + i.astype(F32))
        tab_sa[pl.ds(pl.multiple_of(8 * i, 8), 8)] = fscale[2] * (0.5 * jnp.sin(angle))
        return carry

    lax.fori_loop(0, ROWS_A, table_row, 0)

    def table_ab(i, carry):
        row = lax.broadcasted_iota(jnp.int32, (8, 128), 0).astype(F32) + 8.0 * i.astype(F32)
        a = jnp.floor((row + 0.5) * (1.0 / COLS_B))
        b = row - a * COLS_B
        tab_ab[pl.ds(pl.multiple_of(8 * i, 8), 8)] = fscale[0] * (
            jnp.cos(step_a * (first_a + a)) - 0.5 * jnp.cos(step_b * (first_b + b))
        )
        return carry

    lax.fori_loop(0, 9, table_ab, 0)

    def table_lane(g, carry):
        last = g == GROUPS - 1
        piece = jnp.floor((lane8f + 0.5) * 0.0625)
        plane = jnp.where(last, piece, g.astype(F32))
        spot = jnp.where(last, 128.0 + lane8f - 16.0 * piece, lane8f)
        pair = jnp.floor((spot + 0.5) * 0.5)
        a = jnp.floor((pair + 0.5) * (1.0 / COLS_B))
        b = pair - a * COLS_B
        sin_b = jnp.sin(step_b * (first_b + b))
        x0 = (plane - PLANES / 2 + 0.5) * cell
        keep = plane < 4.0
        where = pl.ds(pl.multiple_of(8 * g, 8), 8)
        tab_l3[where] = jnp.where(keep, fscale[3] * (sin_b - x0), 0.0)
        tab_l4[where] = jnp.where(keep, fscale[4] * (jnp.cos(step_a * (first_a + a)) * sin_b), 0.0)
        return carry

    lax.fori_loop(0, GROUPS, table_lane, 0)
    locals_[0].wait()

    def whole(ref, k):
        return remote(ref, ref, halo_s.at[k], halo_r.at[k], partner)

    halo_refs = (ghost_al, ghost_ah, ghost_bl, ghost_bh, side_in)

    def start_side():
        remote(side_out, side_in, halo_s.at[4], halo_r.at[4], partner).start()

    def start_cols(a):
        at = pl.multiple_of(a * LINE, 8)
        to = pl.ds(pl.multiple_of(a * 72, 8), 72)
        remote(
            val.at[pl.ds(at + 72, 72)], ghost_bl.at[to], halo_s.at[2], halo_r.at[2], col_after
        ).start()
        remote(
            val.at[pl.ds(at, 72)], ghost_bh.at[to], halo_s.at[3], halo_r.at[3], col_before
        ).start()

    def start_high():
        remote(
            val.at[pl.ds((ROWS_A - 3) * LINE, 3 * LINE)], ghost_al,
            halo_s.at[0], halo_r.at[0], row_after,
        ).start()

    def start_low():
        remote(
            val.at[pl.ds(0, 3 * LINE)], ghost_ah, halo_s.at[1], halo_r.at[1], row_before
        ).start()

    def tr_row(g, slot):
        return g * (SLOTS * PITCH) + slot * PITCH

    def to_transposed():
        def put(g, r, block):
            for k in range(16):
                merged = r * 128 + 8 * k
                row = tr_row(g, GHOST + merged // N4) + merged % N4
                tr[pl.ds(row, 8)] = block[8 * k:8 * k + 8]

        def body(g, carry):
            for r in range(3):
                put(g, r, val[pl.ds(r * PLANES + g, 128, stride=12)].T)
            return carry

        lax.fori_loop(0, GROUPS - 1, body, 0)
        for r in range(3):
            parts = [
                val[pl.ds(1536 + r * PLANES + p, 16, stride=12)] for p in range(PLANES)
            ]
            parts.append(jnp.zeros((64, 128), F32))
            put(GROUPS - 1, r, jnp.concatenate(parts, axis=0).T)

    is_low = half == 0
    turn = jnp.where(is_low, 127, 1)
    mine = jnp.where(is_low, lane8 & 1, 1 - (lane8 & 1)) == 0
    send_slot = jnp.where(is_low, GHOST + 5, GHOST)

    def pack_side():
        def body(k, carry):
            for s in range(3):
                for q in range(6):
                    one = tr[pl.ds(tr_row(2 * k, send_slot + s) + 8 * q, 8)]
                    two = tr[pl.ds(tr_row(jnp.minimum(2 * k + 1, 4), send_slot + s) + 8 * q, 8)]
                    side_out[pl.ds(k * 144 + s * 48 + 8 * q, 8)] = jnp.where(
                        mine, pltpu.roll(one, turn, 1), two
                    )
            return carry

        lax.fori_loop(0, 3, body, 0)

    def merge_side():
        def body(g, carry):
            pack = lax.div(g, 2)
            second = lax.rem(g, 2) == 1
            back = jnp.where(is_low, 1, 127)
            for s in range(3):
                for q in range(6):
                    at = 8 * q
                    got = side_in[pl.ds(pack * 144 + s * 48 + at, 8)]
                    got = jnp.where(second, pltpu.roll(got, back, 1), got)
                    top = tr[pl.ds(tr_row(g, GHOST + 7) + at, 8)]
                    bottom = tr[pl.ds(tr_row(g, GHOST) + at, 8)]
                    up = pltpu.roll(tr[pl.ds(tr_row(g, GHOST + s) + at, 8)], 127, 1)
                    down = pltpu.roll(tr[pl.ds(tr_row(g, GHOST + 5 + s) + at, 8)], 1, 1)
                    tr[pl.ds(tr_row(g, GHOST + 8 + s) + at, 8)] = jnp.where(
                        odd, jnp.where(is_low, got, top), up
                    )
                    tr[pl.ds(tr_row(g, s) + at, 8)] = jnp.where(
                        odd, down, jnp.where(is_low, bottom, got)
                    )
            return carry

        lax.fori_loop(0, GROUPS, body, 0)

    def cell_out(left, right, flow, square, factor, peak):
        total = left + right
        gap = right - left
        rest = flow - total
        peak = jnp.maximum(peak, jnp.abs(rest) + jnp.abs(gap))
        return gap, (square - rest * rest) * factor, peak

    zero = jnp.zeros((8, 128), F32)

    def along_planes(first, end, peak):
        def body(n, peak):
            i, c = lax.div(n, CHUNKS), lax.rem(n, CHUNKS)
            q = jnp.where(i < 4, half * 5 + i, jnp.where(i == 4, 4, other * 5 + i - 5))
            start = q * (8 * CELL) + c * PLANES
            rows = [pl.ds(start + p, 8, stride=CELL) for p in range(PLANES)]
            got = [val[rows[p]] for p in range(PLANES)]
            flow = tab_ab[pl.ds(pl.multiple_of(8 * q, 8), 8)] + tab_x3[
                pl.ds(pl.multiple_of(8 * c, 8), 8)
            ]
            square = flow * flow
            line = [got[0]] * 3 + got + [got[3]] * 3
            for p, (left, right) in enumerate(chain(line)):
                left = zero if left is None else left
                right = zero if right is None else right
                gap, part, peak = cell_out(left, right, flow, square, kk[0], peak)
                d_p[rows[p]] = gap
                hn[rows[p]] = part
            return peak

        return lax.fori_loop(first * CHUNKS, end * CHUNKS, body, peak)

    def along_rows():
        def body(n, peak):
            at = pl.multiple_of(8 * n, 8)
            line = (
                [ghost_al[pl.ds(i * LINE + at, 8)] for i in range(3)]
                + [val[pl.ds(a * LINE + at, 8)] for a in range(ROWS_A)]
                + [ghost_ah[pl.ds(i * LINE + at, 8)] for i in range(3)]
            )
            flow = tab_f1[pl.ds(pl.multiple_of(8 * lax.rem(n, 3), 8), 8)]
            square = flow * flow
            for a, (left, right) in enumerate(chain(line)):
                gap, part, peak = cell_out(left, right, flow, square, kk[1], peak)
                where = pl.ds(a * LINE + at, 8)
                d_a[where] = gap
                hn[where] += part
            return peak

        return lax.fori_loop(0, LINE // 8, body, zero)

    def along_cols():
        def body(n, peak):
            a, j = lax.div(n, 3), lax.rem(n, 3)
            ghost = pl.multiple_of(a * 72 + 8 * j, 8)
            at = pl.multiple_of(a * LINE + 8 * j, 8)
            line = (
                [ghost_bl[pl.ds(ghost + i * CELL, 8)] for i in range(3)]
                + [val[pl.ds(at + b * CELL, 8)] for b in range(COLS_B)]
                + [ghost_bh[pl.ds(ghost + i * CELL, 8)] for i in range(3)]
            )
            flow = tab_f2[pl.ds(pl.multiple_of(8 * j, 8), 8)] + tab_sa[
                pl.ds(pl.multiple_of(8 * a, 8), 8)
            ]
            square = flow * flow
            for b, (left, right) in enumerate(chain(line)):
                gap, part, peak = cell_out(left, right, flow, square, kk[2], peak)
                where = pl.ds(at + b * CELL, 8)
                d_b[where] = gap
                hn[where] += part
            return peak

        return lax.fori_loop(0, 3 * ROWS_A, body, zero)

    def along_third():
        def body(n, peak):
            g, q = lax.div(n, 6), lax.rem(n, 6)
            line = [tr[pl.ds(tr_row(g, s) + 8 * q, 8)] for s in range(SLOTS)]
            flow = tab_l3[pl.ds(pl.multiple_of(8 * g, 8), 8)]
            square = flow * flow
            for s, (left, right) in enumerate(chain(line)):
                gap, part, peak = cell_out(left, right, flow, square, kk[3], peak)
                where = pl.ds((g * 8 + s) * PITCH + 8 * q, 8)
                d_3[where] = gap
                ht[where] += part
            return peak

        return lax.fori_loop(0, GROUPS * 6, body, zero)

    slope4 = fscale[4] * cell

    def along_fourth():
        def body(n, peak):
            g, seg = lax.div(n, 4), lax.rem(n, 4)
            first = seg * 12
            line = []
            for i in range(-3, 15):
                at = first + i
                if i < 0:
                    at = jnp.maximum(at, 0)
                if i > 11:
                    at = jnp.minimum(at, N4 - 1)
                line.append(tr[pl.ds(tr_row(g, GHOST) + at, 8, stride=PITCH)])
            table = tab_l4[pl.ds(pl.multiple_of(8 * g, 8), 8)]
            base = table - slope4 * (first.astype(F32) - (N4 / 2 - 0.5))
            for i, (left, right) in enumerate(chain(line)):
                flow = base - slope4 * float(i)
                gap, part, peak = cell_out(left, right, flow, flow * flow, kk[4], peak)
                where = pl.ds(g * 8 * PITCH + first + i, 8, stride=PITCH)
                d_4[where] = gap
                ht[where] = part
            return peak

        return lax.fori_loop(0, GROUPS * 4, body, zero)

    def greet(k):
        if k < len(ROUNDS):
            devices = [(lax.rem(gx + dx, 8), lax.rem(gy + dy, 16)) for dx, dy in ROUNDS[k]]
        else:
            devices = [partner]
        for device in devices:
            pl.semaphore_signal(met.at[k], inc=1, device_id=device, device_id_type=MESH)

    def met_all(k):
        pl.semaphore_wait(met.at[k], len(ROUNDS[k]) if k < len(ROUNDS) else 1)

    def speeds(step, peaks):
        row = jnp.zeros((1, 128), F32)
        lane = lax.broadcasted_iota(jnp.int32, (1, 128), 1)
        for i, peak in enumerate(peaks):
            row = jnp.where(lane == i, jnp.max(peak), row)
        ar_src[step] = row
        ar_buf[step, me] = row

        for dx, dy in FAR_FIRST:
            remote(
                ar_src.at[step], ar_buf.at[step, me], ar_s.at[step], ar_r.at[step],
                (lax.rem(gx + dx, 8), lax.rem(gy + dy, 16)),
            ).start()

    def all_speeds(step):
        every = ar_buf.at[step, pl.ds(0, 127)]
        whole_row = remote(every, every, ar_s.at[step], ar_r.at[step], partner)
        whole_row.wait_recv()
        best = jnp.max(ar_buf[step], axis=0)
        whole_row.wait_send()
        speed = []
        for i in range(5):
            lane_max = jnp.broadcast_to(best[:, i:i + 1], (8, 128))
            speed.append(lane_max * (costs[i] * (1.0 / 12.0)))
        summed = zero
        for i in range(5):
            summed = summed + speed[i] / SPACING[i]
        time_step = 0.5 / (summed + 1e-6)
        steps_out[step] = time_step[0, 0]
        return time_step, [
            time_step * speed[i] * (1.0 / (12.0 * SPACING[i])) for i in range(5)
        ]

    def from_transposed(dt, coef):
        def take(g, r):
            parts = []
            for k in range(16):
                merged = r * 128 + 8 * k
                row = (g * 8 + merged // N4) * PITCH + merged % N4
                where = pl.ds(row, 8)
                parts.append(coef[3] * d_3[where] + coef[4] * d_4[where] - dt * ht[where])
            return jnp.concatenate(parts, axis=0).T

        def body(g, carry):
            for r in range(3):
                wn[pl.ds(r * PLANES + g, 128, stride=12)] = take(g, r)
            return carry

        lax.fori_loop(0, GROUPS - 1, body, 0)
        for r in range(3):
            block = take(GROUPS - 1, r)
            for p in range(PLANES):
                wn[pl.ds(1536 + r * PLANES + p, 16, stride=12)] = block[16 * p:16 * p + 16]

    def new_line(a, dt, coef):
        for i in range(LINE // 8):
            where = pl.ds(pl.multiple_of(a * LINE + 8 * i, 8), 8)
            moved = val[where] + wn[where] - dt * hn[where]
            moved = moved + coef[0] * d_p[where] + coef[1] * d_a[where] + coef[2] * d_b[where]
            val[where] = jnp.maximum(jnp.minimum(moved, hi[where]), lo[where])

    def update(dt, coef):
        def line_of(n):
            return jnp.where(n < 6, jnp.where(n < 3, n, n + 6), n - 3)

        def body(n, carry):
            new_line(line_of(n), dt, coef)

            @pl.when(n > 0)
            def _():
                start_cols(line_of(n - 1))

            @pl.when(n == 3)
            def _():
                start_low()

            @pl.when(n == 6)
            def _():
                start_high()

            return carry

        lax.fori_loop(0, ROWS_A, body, 0)
        start_cols(8)

    def last_update(dt, coef):
        def move(a, launch):
            launch(cells_of(val, a * COLS_B, COLS_B), pl.ds(lax.rem(a, 6) * COLS_B, COLS_B))

        mine_out = pl.ds(pl.multiple_of(half * CELL, 8), CELL)

        def far(src, to):
            remote(src, out_hbm.at[to, mine_out], out_s, out_r, partner).start()

        def near(src, to):
            pltpu.make_async_copy(src, out_hbm.at[to, mine_out], out_sem).start()

        for first, launch in ((other * 6, far), (half * 6, near)):
            def body(n, carry, first=first, launch=launch):
                new_line(first + n, dt, coef)

                @pl.when(n > 0)
                def _():
                    move(first + n - 1, launch)

                return carry

            lax.fori_loop(0, 6, body, 0)
            move(first + 5, launch)
        pltpu.make_async_copy(
            cells_of(val, half * 36, 36), part_of(out_hbm, half), out_sem
        ).wait()
        sent = remote(
            cells_of(val, other * 36, 36), part_of(out_hbm, other), out_s, out_r, partner
        )
        sent.wait_send()
        sent.wait_recv()

    def bounds():
        def body(n, carry):
            for i in range(6):
                where = pl.ds(pl.multiple_of(48 * n + 8 * i, 8), 8)
                hi[where] = jnp.where(mask_t[where] == 1, -0.5, BIG)
                lo[where] = jnp.where(mask_o[where] == 1, 0.5, -BIG)
            return carry

        lax.fori_loop(0, TOTAL // 48, body, 0)

    def own_cols(a, carry):
        start_cols(half * 6 + a)
        return carry

    def other_cols(a, carry):
        start_cols(other * 6 + a)
        return carry

    lax.fori_loop(0, 6, own_cols, 0)
    greet(0)
    early = along_planes(0, 4, zero)
    met_all(0)
    greet(1)
    swaps[0].wait_recv()
    lax.fori_loop(0, 6, other_cols, 0)
    start_low()
    start_high()

    for step in range(STEPS):
        to_transposed()
        pack_side()
        start_side()
        if step == 0:
            swaps[1].start()
            peak_p = along_planes(4, 9, early)
            met_all(1)
            greet(2)
        else:
            peak_p = along_planes(0, 9, zero)
        peak_4 = along_fourth()
        if step == 0:
            met_all(2)
            greet(3)
        whole(ghost_al, 0).wait_recv()
        whole(ghost_ah, 1).wait_recv()
        peak_a = along_rows()
        if step == 0:
            met_all(3)
            greet(4)
        whole(ghost_bl, 2).wait_recv()
        whole(ghost_bh, 3).wait_recv()
        peak_b = along_cols()
        if step == 0:
            met_all(4)
            greet(5)
        whole(side_in, 4).wait_recv()
        merge_side()
        peak_3 = along_third()
        if step == 0:
            met_all(5)
        speeds(step, [peak_p, peak_a, peak_b, peak_3, peak_4])
        for k, ref in enumerate(halo_refs):
            whole(ref, k).wait_send()
        if step == 0:
            swaps[2].start()
        dt, coef = all_speeds(step)
        from_transposed(dt, coef)
        if step == 0:
            for k in (1, 2):
                locals_[k].wait()
                swaps[k].wait_recv()
            bounds()
            for k in range(3):
                swaps[k].wait_send()
        if step < STEPS - 1:
            update(dt, coef)
        else:
            last_update(dt, coef)


def to_rows(x):
    x = x.transpose(1, 2, 0, 3).reshape(6, 6, PLANES, 12, 128)
    return x.transpose(0, 1, 3, 2, 4).reshape(36, 48, 128)


def from_rows(x):
    x = x.reshape(6, 6, 12, PLANES, 128).transpose(0, 1, 3, 2, 4)
    return x.reshape(6, 6, PLANES, 1536).transpose(2, 0, 1, 3)


def solution(mesh):
    def rows(n):
        return pltpu.VMEM((n, 128), F32)

    dma = pltpu.SemaphoreType.DMA
    trans = GROUPS * 8 * PITCH
    scratch = [
        rows(TOTAL), rows(TOTAL), rows(TOTAL), rows(TOTAL), rows(TOTAL), rows(TOTAL),
        rows(TOTAL), rows(TOTAL),
        rows(3 * LINE), rows(3 * LINE), rows(ROWS_A * 72), rows(ROWS_A * 72),
        rows(GROUPS * SLOTS * PITCH), rows(trans), rows(trans), rows(trans),
        rows(432), rows(432),
        pltpu.VMEM((TOTAL, 128), jnp.int32), pltpu.VMEM((TOTAL, 128), jnp.int32),
        rows(24), rows(24), rows(8 * ROWS_A), rows(72), rows(8 * CHUNKS),
        rows(8 * GROUPS), rows(8 * GROUPS),
        pltpu.VMEM((STEPS, 1, 128), F32), pltpu.VMEM((STEPS, 128, 1, 128), F32),
        pltpu.SemaphoreType.REGULAR((6,)),
        dma((3,)), dma((3,)), dma((3,)), dma((5,)), dma((5,)), dma((STEPS,)), dma((STEPS,)),
        dma(()), dma(()), dma(()),
    ]

    def body(value_field, target_mask, obstacle_mask, drift_gains, control_costs):
        anywhere = pl.BlockSpec(memory_space=pl.ANY)
        scalars = pl.BlockSpec(memory_space=pltpu.SMEM)
        moved, steps = pl.pallas_call(
            kernel,
            out_shape=(
                jax.ShapeDtypeStruct((36, 48, 128), F32),
                jax.ShapeDtypeStruct((STEPS,), F32),
            ),
            in_specs=[anywhere, anywhere, anywhere, scalars, scalars],
            out_specs=(anywhere, scalars),
            scratch_shapes=scratch,
            compiler_params=pltpu.CompilerParams(
                collective_id=0, has_side_effects=True, vmem_limit_bytes=56 * 2**20
            ),
        )(
            to_rows(value_field), to_rows(target_mask), to_rows(obstacle_mask),
            drift_gains, control_costs,
        )
        return from_rows(moved), steps

    grid = P(None, "gx", "gy", None)
    return jax.shard_map(
        body, mesh=mesh, in_specs=(grid, grid, grid, P(), P()), out_specs=(grid, P()),
        check_vma=False,
    )
```

```python
import functools
import math

import jax
import jax.numpy as jnp
from jax import lax
from jax.experimental import pallas as pl
from jax.experimental.pallas import tpu as pltpu
from jax.experimental.layout import Layout, with_layout_constraint
from jax.sharding import PartitionSpec as P

PLANES, N3, N4, GRID, STEPS, NA, NB = 4, 32, 48, 96, 3, 48, 96
SPACING = (2.0 / GRID, 2.0 * math.pi / NA, 2.0 * math.pi / NB, 2.0 / GRID, 2.0 / GRID)
MESH = pl.DeviceIdType.MESH
F32 = jnp.float32
BIG = 3.0e38

ROWS_A, COLS_B, CHUNKS = 12, 6, 6
CELL = PLANES * CHUNKS
LINE = COLS_B * CELL
TOTAL = ROWS_A * LINE
GROUPS = 5
PITCH = 52
SLOTS = 14
GHOST = 3
EPS = 0.75e-6


def _hops(offset):
    dx, dy = offset
    ring = lambda n: min(n, 4 - n)
    return ring(dx // 2) + 2 * (dx % 2) + ring(dy // 2 % 4) + dy // 8


FAR_FIRST = sorted(
    [(dx, dy) for dx in range(8) for dy in range(16) if dx or dy], key=_hops, reverse=True
)
ROUNDS = (((0, 1), (0, 15)), ((0, 2), (0, 14)), ((0, 4), (0, 12)), ((2, 0), (6, 0)), ((4, 0),))


def _add(x, y):
    if x is None:
        return y
    if y is None:
        return x
    return x + y


def _sub(x, y):
    if y is None:
        return x
    if x is None:
        return -y
    return x - y


def _mul(x, y):
    if x is None or y is None:
        return None
    return x * y


def chain(values):
    cells = len(values) - 6
    diffs = [
        None if values[i] is values[i + 1] else values[i + 1] - values[i]
        for i in range(cells + 5)
    ]
    curve, twice, lean, weight_x, weight_y, weight_z = {}, {}, {}, {}, {}, {}
    previous = None

    def curve_at(i):
        if i not in curve:
            curve[i] = _sub(diffs[i + 1], diffs[i])
            twice[i] = _add(curve[i], curve[i])
            square = _mul(curve[i], curve[i])
            lean[i] = (square, _mul(square, 1.5))
        return curve[i]

    def smooth_at(i):
        if i not in weight_x:
            now, last = curve_at(i), curve_at(i - 1)
            cross = _mul(now, last)
            base = _add(lean[i][0], lean[i - 1][0])
            base = EPS if base is None else base + EPS
            middle = _sub(base, _mul(cross, 2.75))
            x = _add(middle, lean[i][1])
            y = _add(middle, lean[i - 1][1])
            z = _add(middle, _mul(cross, 1.5))
            weight_x[i], weight_y[i], weight_z[i] = x * x, y * y, z * z

    def third_at(i):
        return _sub(_add(curve_at(i + 1), curve_at(i - 1)), twice[i])

    thirds = {}
    for face in range(2, cells + 3):
        for i in (face - 1, face, face + 1):
            smooth_at(i)
        one, two, three = weight_x[face - 1], weight_z[face], weight_y[face + 1]
        w_low, w_mid, w_high = two * three, one * three, one * two
        for i in (face - 1, face):
            if i not in thirds:
                thirds[i] = third_at(i)
        low = _mul(thirds[face - 1], w_low)
        high = _mul(thirds[face], w_high)
        base = ((w_low + w_high) + (w_mid + w_mid)) * 1.5
        now, last = curve[face], curve[face - 1]
        scaled = _mul(diffs[face], 6.0)
        left = right = None
        if face < cells + 2:
            top = _add(low, _mul(high, 1.5))
            left = _add(scaled, _add(last, twice[face]))
            if top is not None:
                left = _sub(left, top * pl.reciprocal(base - w_low, approx=True))
        if face > 2:
            top = _add(_mul(low, 1.5), high)
            right = _sub(scaled, _add(now, twice[face - 1]))
            if top is not None:
                right = _add(right, top * pl.reciprocal(base - w_high, approx=True))
            yield previous, right
        previous = left


def kernel(
    value_hbm, target_hbm, obstacle_hbm, gains, costs,
    out_hbm, steps_out,
    val, hn, d_a, d_b, d_p, wn, hi, lo,
    ghost_al, ghost_ah, ghost_bl, ghost_bh,
    tr, ht, d_3, d_4, side_out, side_in,
    mask_t, mask_o,
    tab_f1, tab_f2, tab_sa, tab_ab, tab_x3, tab_l3, tab_l4,
    ar_src, ar_buf,
    met, local_sem, swap_s, swap_r, halo_s, halo_r, ar_s, ar_r, out_sem, out_s, out_r,
):
    gx, gy = lax.axis_index("gx"), lax.axis_index("gy")
    half = lax.rem(gx, 2)
    other = 1 - half
    partner = (gx + 1 - 2 * half, gy)
    me = gx * 16 + gy

    def remote(src, dst, send, recv, device):
        return pltpu.make_async_remote_copy(
            src_ref=src, dst_ref=dst, send_sem=send, recv_sem=recv,
            device_id=device, device_id_type=MESH,
        )

    row_before = (lax.rem(gx + 6, 8), gy)
    row_after = (lax.rem(gx + 2, 8), gy)
    col_before = (gx, lax.rem(gy + 15, 16))
    col_after = (gx, lax.rem(gy + 1, 16))
    barrier = pltpu.get_barrier_semaphore()
    for device in (partner, col_before, col_after, row_before, row_after):
        pl.semaphore_signal(barrier, inc=1, device_id=device, device_id_type=MESH)

    def part_of(ref, which):
        return ref.at[:, pl.ds(pl.multiple_of(which * CELL, 8), CELL)]

    inputs = (value_hbm, target_hbm, obstacle_hbm)
    places = (val, mask_t, mask_o)

    def cells_of(ref, first, count):
        return ref.reshape(TOTAL // CELL, CELL, 128).at[pl.ds(first, count)]

    swaps = [
        remote(
            part_of(inputs[k], other), cells_of(places[k], half * 36, 36),
            swap_s.at[k], swap_r.at[k], partner,
        )
        for k in range(3)
    ]
    locals_ = [
        pltpu.make_async_copy(
            part_of(inputs[k], half), cells_of(places[k], half * 36, 36), local_sem.at[k]
        )
        for k in range(3)
    ]
    for k in range(3):
        locals_[k].start()
    pl.semaphore_wait(barrier, 5)
    swaps[0].start()

    lane8 = lax.broadcasted_iota(jnp.int32, (8, 128), 1)
    lane8f = lane8.astype(F32)
    odd = (lane8 & 1) == 1

    def splat(scalar):
        return jnp.full((8, 128), scalar, F32)

    fscale = [splat(12.0 * gains[i]) / splat(costs[i]) for i in range(5)]
    kk = [costs[i] * (1.0 / (288.0 * SPACING[i])) for i in range(5)]
    half_f = half.astype(F32)
    first_a = (lax.div(gx, 2) * ROWS_A).astype(F32)
    first_b = (gy * COLS_B).astype(F32)
    step_a, step_b = 2.0 * math.pi / NA, 2.0 * math.pi / NB
    cell = 2.0 / GRID

    def split_lane(merged):
        third = jnp.floor((merged + 0.5) * (1.0 / N4))
        return third, merged - third * N4

    for block in range(3):
        row = lax.broadcasted_iota(jnp.int32, (8, 128), 0).astype(F32) + 8.0 * block
        chunk = jnp.floor((row + 0.5) * (1.0 / PLANES))
        plane = row - chunk * PLANES
        merged = (half_f * CHUNKS + chunk) * 128.0 + lane8f
        third, fourth = split_lane(merged)
        x0 = (plane - PLANES / 2 + 0.5) * cell
        x3 = (third - N3 / 2 + 0.5) * cell
        x4 = (fourth - N4 / 2 + 0.5) * cell
        tab_f1[pl.ds(8 * block, 8)] = fscale[1] * (x4 - 0.3 * x0)
        tab_f2[pl.ds(8 * block, 8)] = fscale[2] * x3
    for chunk in range(CHUNKS):
        third, _ = split_lane((half_f * CHUNKS + chunk) * 128.0 + lane8f)
        tab_x3[pl.ds(8 * chunk, 8)] = fscale[0] * ((third - N3 / 2 + 0.5) * cell)

    def table_row(i, carry):
        angle = step_a * (splat(first_a) + i.astype(F32))
        tab_sa[pl.ds(pl.multiple_of(8 * i, 8), 8)] = fscale[2] * (0.5 * jnp.sin(angle))
        return carry

    lax.fori_loop(0, ROWS_A, table_row, 0)

    def table_ab(i, carry):
        row = lax.broadcasted_iota(jnp.int32, (8, 128), 0).astype(F32) + 8.0 * i.astype(F32)
        a = jnp.floor((row + 0.5) * (1.0 / COLS_B))
        b = row - a * COLS_B
        tab_ab[pl.ds(pl.multiple_of(8 * i, 8), 8)] = fscale[0] * (
            jnp.cos(step_a * (first_a + a)) - 0.5 * jnp.cos(step_b * (first_b + b))
        )
        return carry

    lax.fori_loop(0, 9, table_ab, 0)

    def table_lane(g, carry):
        last = g == GROUPS - 1
        piece = jnp.floor((lane8f + 0.5) * 0.0625)
        plane = jnp.where(last, piece, g.astype(F32))
        spot = jnp.where(last, 128.0 + lane8f - 16.0 * piece, lane8f)
        pair = jnp.floor((spot + 0.5) * 0.5)
        a = jnp.floor((pair + 0.5) * (1.0 / COLS_B))
        b = pair - a * COLS_B
        sin_b = jnp.sin(step_b * (first_b + b))
        x0 = (plane - PLANES / 2 + 0.5) * cell
        keep = plane < 4.0
        where = pl.ds(pl.multiple_of(8 * g, 8), 8)
        tab_l3[where] = jnp.where(keep, fscale[3] * (sin_b - x0), 0.0)
        tab_l4[where] = jnp.where(keep, fscale[4] * (jnp.cos(step_a * (first_a + a)) * sin_b), 0.0)
        return carry

    lax.fori_loop(0, GROUPS, table_lane, 0)
    locals_[0].wait()

    def whole(ref, k):
        return remote(ref, ref, halo_s.at[k], halo_r.at[k], partner)

    halo_refs = (ghost_al, ghost_ah, ghost_bl, ghost_bh, side_in)

    def start_side():
        remote(side_out, side_in, halo_s.at[4], halo_r.at[4], partner).start()

    def start_cols(a):
        at = pl.multiple_of(a * LINE, 8)
        to = pl.ds(pl.multiple_of(a * 72, 8), 72)
        remote(
            val.at[pl.ds(at + 72, 72)], ghost_bl.at[to], halo_s.at[2], halo_r.at[2], col_after
        ).start()
        remote(
            val.at[pl.ds(at, 72)], ghost_bh.at[to], halo_s.at[3], halo_r.at[3], col_before
        ).start()

    def start_high():
        remote(
            val.at[pl.ds((ROWS_A - 3) * LINE, 3 * LINE)], ghost_al,
            halo_s.at[0], halo_r.at[0], row_after,
        ).start()

    def start_low():
        remote(
            val.at[pl.ds(0, 3 * LINE)], ghost_ah, halo_s.at[1], halo_r.at[1], row_before
        ).start()

    def tr_row(g, slot):
        return g * (SLOTS * PITCH) + slot * PITCH

    def to_transposed():
        def put(g, r, block):
            for k in range(16):
                merged = r * 128 + 8 * k
                row = tr_row(g, GHOST + merged // N4) + merged % N4
                tr[pl.ds(row, 8)] = block[8 * k:8 * k + 8]

        for g in range(GROUPS - 1):
            for r in range(3):
                put(g, r, val[pl.ds(r * PLANES + g, 128, stride=12)].T)
        for r in range(3):
            parts = [
                val[pl.ds(1536 + r * PLANES + p, 16, stride=12)] for p in range(PLANES)
            ]
            parts.append(jnp.zeros((64, 128), F32))
            put(GROUPS - 1, r, jnp.concatenate(parts, axis=0).T)

    is_low = half == 0
    turn = jnp.where(is_low, 127, 1)
    mine = jnp.where(is_low, lane8 & 1, 1 - (lane8 & 1)) == 0
    send_slot = jnp.where(is_low, GHOST + 5, GHOST)

    def pack_side():
        def body(k, carry):
            for s in range(3):
                for q in range(6):
                    one = tr[pl.ds(tr_row(2 * k, send_slot + s) + 8 * q, 8)]
                    two = tr[pl.ds(tr_row(jnp.minimum(2 * k + 1, 4), send_slot + s) + 8 * q, 8)]
                    side_out[pl.ds(k * 144 + s * 48 + 8 * q, 8)] = jnp.where(
                        mine, pltpu.roll(one, turn, 1), two
                    )
            return carry

        lax.fori_loop(0, 3, body, 0, unroll=True)

    def merge_side():
        def body(g, carry):
            pack = lax.div(g, 2)
            second = lax.rem(g, 2) == 1
            back = jnp.where(is_low, 1, 127)
            for s in range(3):
                for q in range(6):
                    at = 8 * q
                    got = side_in[pl.ds(pack * 144 + s * 48 + at, 8)]
                    got = jnp.where(second, pltpu.roll(got, back, 1), got)
                    top = tr[pl.ds(tr_row(g, GHOST + 7) + at, 8)]
                    bottom = tr[pl.ds(tr_row(g, GHOST) + at, 8)]
                    up = pltpu.roll(tr[pl.ds(tr_row(g, GHOST + s) + at, 8)], 127, 1)
                    down = pltpu.roll(tr[pl.ds(tr_row(g, GHOST + 5 + s) + at, 8)], 1, 1)
                    tr[pl.ds(tr_row(g, GHOST + 8 + s) + at, 8)] = jnp.where(
                        odd, jnp.where(is_low, got, top), up
                    )
                    tr[pl.ds(tr_row(g, s) + at, 8)] = jnp.where(
                        odd, down, jnp.where(is_low, bottom, got)
                    )
            return carry

        lax.fori_loop(0, GROUPS, body, 0, unroll=True)

    def cell_out(left, right, flow, square, factor, peak):
        total = left + right
        gap = right - left
        rest = flow - total
        peak = jnp.maximum(peak, jnp.abs(rest) + jnp.abs(gap))
        return gap, (square - rest * rest) * factor, peak

    zero = jnp.zeros((8, 128), F32)

    def along_planes(first, end, peak):
        def body(n, peak):
            i, c = lax.div(n, CHUNKS), lax.rem(n, CHUNKS)
            q = jnp.where(i < 4, half * 5 + i, jnp.where(i == 4, 4, other * 5 + i - 5))
            start = q * (8 * CELL) + c * PLANES
            rows = [pl.ds(start + p, 8, stride=CELL) for p in range(PLANES)]
            got = [val[rows[p]] for p in range(PLANES)]
            flow = tab_ab[pl.ds(pl.multiple_of(8 * q, 8), 8)] + tab_x3[
                pl.ds(pl.multiple_of(8 * c, 8), 8)
            ]
            square = flow * flow
            line = [got[0]] * 3 + got + [got[3]] * 3
            for p, (left, right) in enumerate(chain(line)):
                left = zero if left is None else left
                right = zero if right is None else right
                gap, part, peak = cell_out(left, right, flow, square, kk[0], peak)
                d_p[rows[p]] = gap
                hn[rows[p]] = part
            return peak

        return lax.fori_loop(first * CHUNKS, end * CHUNKS, body, peak, unroll=2)

    def along_rows():
        def body(n, peak):
            at = pl.multiple_of(8 * n, 8)
            line = (
                [ghost_al[pl.ds(i * LINE + at, 8)] for i in range(3)]
                + [val[pl.ds(a * LINE + at, 8)] for a in range(ROWS_A)]
                + [ghost_ah[pl.ds(i * LINE + at, 8)] for i in range(3)]
            )
            flow = tab_f1[pl.ds(pl.multiple_of(8 * lax.rem(n, 3), 8), 8)]
            square = flow * flow
            for a, (left, right) in enumerate(chain(line)):
                gap, part, peak = cell_out(left, right, flow, square, kk[1], peak)
                where = pl.ds(a * LINE + at, 8)
                d_a[where] = gap
                hn[where] += part
            return peak

        return lax.fori_loop(0, LINE // 8, body, zero, unroll=1)

    def along_cols():
        def body(n, peak):
            a, j = lax.div(n, 3), lax.rem(n, 3)
            ghost = pl.multiple_of(a * 72 + 8 * j, 8)
            at = pl.multiple_of(a * LINE + 8 * j, 8)
            line = (
                [ghost_bl[pl.ds(ghost + i * CELL, 8)] for i in range(3)]
                + [val[pl.ds(at + b * CELL, 8)] for b in range(COLS_B)]
                + [ghost_bh[pl.ds(ghost + i * CELL, 8)] for i in range(3)]
            )
            flow = tab_f2[pl.ds(pl.multiple_of(8 * j, 8), 8)] + tab_sa[
                pl.ds(pl.multiple_of(8 * a, 8), 8)
            ]
            square = flow * flow
            for b, (left, right) in enumerate(chain(line)):
                gap, part, peak = cell_out(left, right, flow, square, kk[2], peak)
                where = pl.ds(at + b * CELL, 8)
                d_b[where] = gap
                hn[where] += part
            return peak

        return lax.fori_loop(0, 3 * ROWS_A, body, zero, unroll=2)

    def along_third():
        def body(n, peak):
            g, q = lax.div(n, 6), lax.rem(n, 6)
            line = [tr[pl.ds(tr_row(g, s) + 8 * q, 8)] for s in range(SLOTS)]
            flow = tab_l3[pl.ds(pl.multiple_of(8 * g, 8), 8)]
            square = flow * flow
            for s, (left, right) in enumerate(chain(line)):
                gap, part, peak = cell_out(left, right, flow, square, kk[3], peak)
                where = pl.ds((g * 8 + s) * PITCH + 8 * q, 8)
                d_3[where] = gap
                ht[where] += part
            return peak

        return lax.fori_loop(0, GROUPS * 6, body, zero, unroll=2)

    slope4 = fscale[4] * cell

    def along_fourth():
        def body(n, peak):
            g, seg = lax.div(n, 4), lax.rem(n, 4)
            first = seg * 12
            line = []
            for i in range(-3, 15):
                at = first + i
                if i < 0:
                    at = jnp.maximum(at, 0)
                if i > 11:
                    at = jnp.minimum(at, N4 - 1)
                line.append(tr[pl.ds(tr_row(g, GHOST) + at, 8, stride=PITCH)])
            table = tab_l4[pl.ds(pl.multiple_of(8 * g, 8), 8)]
            base = table - slope4 * (first.astype(F32) - (N4 / 2 - 0.5))
            for i, (left, right) in enumerate(chain(line)):
                flow = base - slope4 * float(i)
                gap, part, peak = cell_out(left, right, flow, flow * flow, kk[4], peak)
                where = pl.ds(g * 8 * PITCH + first + i, 8, stride=PITCH)
                d_4[where] = gap
                ht[where] = part
            return peak

        return lax.fori_loop(0, GROUPS * 4, body, zero, unroll=1)

    def greet(k):
        if k < len(ROUNDS):
            devices = [(lax.rem(gx + dx, 8), lax.rem(gy + dy, 16)) for dx, dy in ROUNDS[k]]
        else:
            devices = [partner]
        for device in devices:
            pl.semaphore_signal(met.at[k], inc=1, device_id=device, device_id_type=MESH)

    def met_all(k):
        pl.semaphore_wait(met.at[k], len(ROUNDS[k]) if k < len(ROUNDS) else 1)

    def speeds(step, peaks):
        row = jnp.zeros((1, 128), F32)
        lane = lax.broadcasted_iota(jnp.int32, (1, 128), 1)
        for i, peak in enumerate(peaks):
            row = jnp.where(lane == i, jnp.max(peak), row)
        ar_src[step] = row
        ar_buf[step, me] = row

        for dx, dy in FAR_FIRST:
            remote(
                ar_src.at[step], ar_buf.at[step, me], ar_s.at[step], ar_r.at[step],
                (lax.rem(gx + dx, 8), lax.rem(gy + dy, 16)),
            ).start()

    def all_speeds(step):
        every = ar_buf.at[step, pl.ds(0, 127)]
        whole_row = remote(every, every, ar_s.at[step], ar_r.at[step], partner)
        whole_row.wait_recv()
        best = jnp.max(ar_buf[step], axis=0)
        whole_row.wait_send()
        speed = []
        for i in range(5):
            lane_max = jnp.broadcast_to(best[:, i:i + 1], (8, 128))
            speed.append(lane_max * (costs[i] * (1.0 / 12.0)))
        summed = zero
        for i in range(5):
            summed = summed + speed[i] / SPACING[i]
        time_step = 0.5 / (summed + 1e-6)
        steps_out[step] = time_step[0, 0]
        return time_step, [
            time_step * speed[i] * (1.0 / (12.0 * SPACING[i])) for i in range(5)
        ]

    def from_transposed(dt, coef):
        def take(g, r):
            parts = []
            for k in range(16):
                merged = r * 128 + 8 * k
                row = (g * 8 + merged // N4) * PITCH + merged % N4
                where = pl.ds(row, 8)
                parts.append(coef[3] * d_3[where] + coef[4] * d_4[where] - dt * ht[where])
            return jnp.concatenate(parts, axis=0).T

        for g in range(GROUPS - 1):
            for r in range(3):
                wn[pl.ds(r * PLANES + g, 128, stride=12)] = take(g, r)
        for r in range(3):
            block = take(GROUPS - 1, r)
            for p in range(PLANES):
                wn[pl.ds(1536 + r * PLANES + p, 16, stride=12)] = block[16 * p:16 * p + 16]

    def new_line(a, dt, coef):
        for i in range(LINE // 8):
            where = pl.ds(pl.multiple_of(a * LINE + 8 * i, 8), 8)
            moved = val[where] + wn[where] - dt * hn[where]
            moved = moved + coef[0] * d_p[where] + coef[1] * d_a[where] + coef[2] * d_b[where]
            val[where] = jnp.maximum(jnp.minimum(moved, hi[where]), lo[where])

    def update(dt, coef):
        def line_of(n):
            return jnp.where(n < 6, jnp.where(n < 3, n, n + 6), n - 3)

        def body(n, carry):
            new_line(line_of(n), dt, coef)

            @pl.when(n > 0)
            def _():
                start_cols(line_of(n - 1))

            @pl.when(n == 3)
            def _():
                start_low()

            @pl.when(n == 6)
            def _():
                start_high()

            return carry

        lax.fori_loop(0, ROWS_A, body, 0)
        start_cols(8)

    def last_update(dt, coef):
        def move(a, launch):
            launch(cells_of(val, a * COLS_B, COLS_B), pl.ds(lax.rem(a, 6) * COLS_B, COLS_B))

        mine_out = pl.ds(pl.multiple_of(half * CELL, 8), CELL)

        def far(src, to):
            remote(src, out_hbm.at[to, mine_out], out_s, out_r, partner).start()

        def near(src, to):
            pltpu.make_async_copy(src, out_hbm.at[to, mine_out], out_sem).start()

        for first, launch in ((other * 6, far), (half * 6, near)):
            def body(n, carry, first=first, launch=launch):
                new_line(first + n, dt, coef)

                @pl.when(n > 0)
                def _():
                    move(first + n - 1, launch)

                return carry

            lax.fori_loop(0, 6, body, 0)
            move(first + 5, launch)
        pltpu.make_async_copy(
            cells_of(val, half * 36, 36), part_of(out_hbm, half), out_sem
        ).wait()
        sent = remote(
            cells_of(val, other * 36, 36), part_of(out_hbm, other), out_s, out_r, partner
        )
        sent.wait_send()
        sent.wait_recv()

    def bounds():
        def body(n, carry):
            for i in range(6):
                where = pl.ds(pl.multiple_of(48 * n + 8 * i, 8), 8)
                hi[where] = jnp.where(mask_t[where] == 1, -0.5, BIG)
                lo[where] = jnp.where(mask_o[where] == 1, 0.5, -BIG)
            return carry

        lax.fori_loop(0, TOTAL // 48, body, 0)

    def own_cols(a, carry):
        start_cols(half * 6 + a)
        return carry

    def other_cols(a, carry):
        start_cols(other * 6 + a)
        return carry

    lax.fori_loop(0, 6, own_cols, 0)
    greet(0)
    early = along_planes(0, 4, zero)
    met_all(0)
    greet(1)
    swaps[0].wait_recv()
    lax.fori_loop(0, 6, other_cols, 0)
    start_low()
    start_high()

    for step in range(STEPS):
        to_transposed()
        pack_side()
        start_side()
        if step == 0:
            swaps[1].start()
            peak_p = along_planes(4, 9, early)
            met_all(1)
            greet(2)
        else:
            peak_p = along_planes(0, 9, zero)
        peak_4 = along_fourth()
        if step == 0:
            met_all(2)
            greet(3)
        whole(ghost_al, 0).wait_recv()
        whole(ghost_ah, 1).wait_recv()
        peak_a = along_rows()
        if step == 0:
            met_all(3)
            greet(4)
        whole(ghost_bl, 2).wait_recv()
        whole(ghost_bh, 3).wait_recv()
        peak_b = along_cols()
        if step == 0:
            met_all(4)
            greet(5)
        whole(side_in, 4).wait_recv()
        merge_side()
        peak_3 = along_third()
        if step == 0:
            met_all(5)
        speeds(step, [peak_p, peak_a, peak_b, peak_3, peak_4])
        for k, ref in enumerate(halo_refs):
            whole(ref, k).wait_send()
        if step == 0:
            swaps[2].start()
        dt, coef = all_speeds(step)
        from_transposed(dt, coef)
        if step == 0:
            for k in (1, 2):
                locals_[k].wait()
                swaps[k].wait_recv()
            bounds()
            for k in range(3):
                swaps[k].wait_send()
        if step < STEPS - 1:
            update(dt, coef)
        else:
            last_update(dt, coef)


def to_rows(x):
    x = x.transpose(1, 2, 0, 3).reshape(6, 6, PLANES, 12, 128)
    x = with_layout_constraint(x, Layout((0, 1, 3, 2, 4)))
    return x.transpose(0, 1, 3, 2, 4).reshape(36, 48, 128)


def from_rows(x):
    x = x.reshape(6, 6, 12, PLANES, 128).transpose(0, 1, 3, 2, 4)
    return x.reshape(6, 6, PLANES, 1536).transpose(2, 0, 1, 3)


def solution(mesh):
    def rows(n):
        return pltpu.VMEM((n, 128), F32)

    dma = pltpu.SemaphoreType.DMA
    trans = GROUPS * 8 * PITCH
    scratch = [
        rows(TOTAL), rows(TOTAL), rows(TOTAL), rows(TOTAL), rows(TOTAL), rows(TOTAL),
        rows(TOTAL), rows(TOTAL),
        rows(3 * LINE), rows(3 * LINE), rows(ROWS_A * 72), rows(ROWS_A * 72),
        rows(GROUPS * SLOTS * PITCH), rows(trans), rows(trans), rows(trans),
        rows(432), rows(432),
        pltpu.VMEM((TOTAL, 128), jnp.int32), pltpu.VMEM((TOTAL, 128), jnp.int32),
        rows(24), rows(24), rows(8 * ROWS_A), rows(72), rows(8 * CHUNKS),
        rows(8 * GROUPS), rows(8 * GROUPS),
        pltpu.VMEM((STEPS, 1, 128), F32), pltpu.VMEM((STEPS, 128, 1, 128), F32),
        pltpu.SemaphoreType.REGULAR((6,)),
        dma((3,)), dma((3,)), dma((3,)), dma((5,)), dma((5,)), dma((STEPS,)), dma((STEPS,)),
        dma(()), dma(()), dma(()),
    ]

    def body(value_field, target_mask, obstacle_mask, drift_gains, control_costs):
        anywhere = pl.BlockSpec(memory_space=pl.ANY)
        scalars = pl.BlockSpec(memory_space=pltpu.SMEM)
        moved, steps = pl.pallas_call(
            kernel,
            out_shape=(
                jax.ShapeDtypeStruct((36, 48, 128), F32),
                jax.ShapeDtypeStruct((STEPS,), F32),
            ),
            in_specs=[anywhere, anywhere, anywhere, scalars, scalars],
            out_specs=(anywhere, scalars),
            scratch_shapes=scratch,
            compiler_params=pltpu.CompilerParams(
                collective_id=0, has_side_effects=True, vmem_limit_bytes=56 * 2**20
            ),
        )(
            to_rows(value_field), to_rows(target_mask), to_rows(obstacle_mask),
            drift_gains, control_costs,
        )
        return from_rows(moved), steps

    grid = P(None, "gx", "gy", None)
    return jax.shard_map(
        body, mesh=mesh, in_specs=(grid, grid, grid, P(), P()), out_specs=(grid, P()),
        check_vma=False,
    )
```

```python
import functools
import math

import jax
import jax.numpy as jnp
from jax import lax
from jax.experimental import pallas as pl
from jax.experimental.pallas import tpu as pltpu
from jax.experimental.layout import Layout, with_layout_constraint
from jax.sharding import PartitionSpec as P

PLANES, N3, N4, GRID, STEPS, NA, NB = 4, 32, 48, 96, 3, 48, 96
SPACING = (2.0 / GRID, 2.0 * math.pi / NA, 2.0 * math.pi / NB, 2.0 / GRID, 2.0 / GRID)
MESH = pl.DeviceIdType.MESH
F32 = jnp.float32
BIG = 3.0e38

ROWS_A, COLS_B, CHUNKS = 12, 6, 6
CELL = PLANES * CHUNKS
LINE = COLS_B * CELL
TOTAL = ROWS_A * LINE
GROUPS = 5
PITCH = 52
SLOTS = 14
GHOST = 3
EPS = 0.75e-6
EARLY = 18


def _hops(offset):
    dx, dy = offset
    ring = lambda n: min(n, 4 - n)
    return ring(dx // 2) + 2 * (dx % 2) + ring(dy // 2 % 4) + dy // 8


FAR_FIRST = sorted(
    [(dx, dy) for dx in range(8) for dy in range(16) if dx or dy], key=_hops, reverse=True
)
ROUNDS = (((0, 1), (0, 15)), ((0, 2), (0, 14)), ((0, 4), (0, 12)), ((2, 0), (6, 0)), ((4, 0),))


def line_order(n):
    return jnp.where(n < 6, jnp.where(n < 3, n, n + 6), n - 3)


def _add(x, y):
    if x is None:
        return y
    if y is None:
        return x
    return x + y


def _sub(x, y):
    if y is None:
        return x
    if x is None:
        return -y
    return x - y


def _mul(x, y):
    if x is None or y is None:
        return None
    return x * y


def chain(values):
    cells = len(values) - 6
    diffs = [
        None if values[i] is values[i + 1] else values[i + 1] - values[i]
        for i in range(cells + 5)
    ]
    curve, twice, lean, weight_x, weight_y, weight_z = {}, {}, {}, {}, {}, {}
    previous = None

    def curve_at(i):
        if i not in curve:
            curve[i] = _sub(diffs[i + 1], diffs[i])
            twice[i] = _add(curve[i], curve[i])
            square = _mul(curve[i], curve[i])
            lean[i] = (square, _mul(square, 1.5))
        return curve[i]

    def smooth_at(i):
        if i not in weight_x:
            now, last = curve_at(i), curve_at(i - 1)
            cross = _mul(now, last)
            base = _add(lean[i][0], lean[i - 1][0])
            base = EPS if base is None else base + EPS
            middle = _sub(base, _mul(cross, 2.75))
            x = _add(middle, lean[i][1])
            y = _add(middle, lean[i - 1][1])
            z = _add(middle, _mul(cross, 1.5))
            weight_x[i], weight_y[i], weight_z[i] = x * x, y * y, z * z

    def third_at(i):
        return _sub(_add(curve_at(i + 1), curve_at(i - 1)), twice[i])

    thirds = {}
    for face in range(2, cells + 3):
        for i in (face - 1, face, face + 1):
            smooth_at(i)
        one, two, three = weight_x[face - 1], weight_z[face], weight_y[face + 1]
        w_low, w_mid, w_high = two * three, one * three, one * two
        for i in (face - 1, face):
            if i not in thirds:
                thirds[i] = third_at(i)
        low = _mul(thirds[face - 1], w_low)
        high = _mul(thirds[face], w_high)
        base = ((w_low + w_high) + (w_mid + w_mid)) * 1.5
        now, last = curve[face], curve[face - 1]
        scaled = _mul(diffs[face], 6.0)
        left = right = None
        if face < cells + 2:
            top = _add(low, _mul(high, 1.5))
            left = _add(scaled, _add(last, twice[face]))
            if top is not None:
                left = _sub(left, top * pl.reciprocal(base - w_low, approx=True))
        if face > 2:
            top = _add(_mul(low, 1.5), high)
            right = _sub(scaled, _add(now, twice[face - 1]))
            if top is not None:
                right = _add(right, top * pl.reciprocal(base - w_high, approx=True))
            yield previous, right
        previous = left


def kernel(
    value_hbm, target_hbm, obstacle_hbm, gains, costs,
    out_hbm, steps_out,
    val, hn, d_a, d_b, d_p, wn, hi, lo,
    ghost_al, ghost_ah, ghost_bl, ghost_bh,
    tr, ht, d_3, d_4, side_out, side_in,
    mask_t, mask_o,
    tab_f1, tab_f2, tab_sa, tab_ab, tab_x3, tab_l3, tab_l4,
    ar_src, ar_buf,
    met, local_sem, swap_s, swap_r, row_s, row_r, col_s, col_r, side_s, side_r, ar_s, ar_r, out_sem, out_s, out_r,
):
    gx, gy = lax.axis_index("gx"), lax.axis_index("gy")
    half = lax.rem(gx, 2)
    other = 1 - half
    partner = (gx + 1 - 2 * half, gy)
    me = gx * 16 + gy

    def remote(src, dst, send, recv, device):
        return pltpu.make_async_remote_copy(
            src_ref=src, dst_ref=dst, send_sem=send, recv_sem=recv,
            device_id=device, device_id_type=MESH,
        )

    row_before = (lax.rem(gx + 6, 8), gy)
    row_after = (lax.rem(gx + 2, 8), gy)
    col_before = (gx, lax.rem(gy + 15, 16))
    col_after = (gx, lax.rem(gy + 1, 16))
    barrier = pltpu.get_barrier_semaphore()
    for device in (partner, col_before, col_after, row_before, row_after):
        pl.semaphore_signal(barrier, inc=1, device_id=device, device_id_type=MESH)

    def part_of(ref, which):
        return ref.at[:, pl.ds(pl.multiple_of(which * CELL, 8), CELL)]

    inputs = (value_hbm, target_hbm, obstacle_hbm)
    places = (val, mask_t, mask_o)

    def cells_of(ref, first, count):
        return ref.reshape(TOTAL // CELL, CELL, 128).at[pl.ds(first, count)]

    def target_of(ref, first, count):
        return ref.at[pl.ds(first, count), pl.ds(pl.multiple_of(other * CELL, 8), CELL)]

    swaps = [
        remote(
            part_of(inputs[k], other), cells_of(places[k], half * 36, 36),
            swap_s.at[k], swap_r.at[k], partner,
        )
        for k in range(2)
    ]
    for k, (first, count) in enumerate(((0, EARLY), (EARLY, 36 - EARLY))):
        swaps.append(
            remote(
                target_of(obstacle_hbm, first, count), cells_of(mask_o, half * 36 + first, count),
                swap_s.at[2 + k], swap_r.at[2 + k], partner,
            )
        )
    locals_ = [
        pltpu.make_async_copy(
            part_of(inputs[k], half), cells_of(places[k], half * 36, 36), local_sem.at[k]
        )
        for k in range(3)
    ]
    for k in range(3):
        locals_[k].start()
    pl.semaphore_wait(barrier, 5)
    swaps[0].start()

    lane8 = lax.broadcasted_iota(jnp.int32, (8, 128), 1)
    lane8f = lane8.astype(F32)
    odd = (lane8 & 1) == 1

    def splat(scalar):
        return jnp.full((8, 128), scalar, F32)

    fscale = [splat(12.0 * gains[i]) / splat(costs[i]) for i in range(5)]
    kk = [costs[i] * (1.0 / (288.0 * SPACING[i])) for i in range(5)]
    half_f = half.astype(F32)
    first_a = (lax.div(gx, 2) * ROWS_A).astype(F32)
    first_b = (gy * COLS_B).astype(F32)
    step_a, step_b = 2.0 * math.pi / NA, 2.0 * math.pi / NB
    cell = 2.0 / GRID

    def split_lane(merged):
        third = jnp.floor((merged + 0.5) * (1.0 / N4))
        return third, merged - third * N4

    for block in range(3):
        row = lax.broadcasted_iota(jnp.int32, (8, 128), 0).astype(F32) + 8.0 * block
        chunk = jnp.floor((row + 0.5) * (1.0 / PLANES))
        plane = row - chunk * PLANES
        merged = (half_f * CHUNKS + chunk) * 128.0 + lane8f
        third, fourth = split_lane(merged)
        x0 = (plane - PLANES / 2 + 0.5) * cell
        x3 = (third - N3 / 2 + 0.5) * cell
        x4 = (fourth - N4 / 2 + 0.5) * cell
        tab_f1[pl.ds(8 * block, 8)] = fscale[1] * (x4 - 0.3 * x0)
        tab_f2[pl.ds(8 * block, 8)] = fscale[2] * x3
    for chunk in range(CHUNKS):
        third, _ = split_lane((half_f * CHUNKS + chunk) * 128.0 + lane8f)
        tab_x3[pl.ds(8 * chunk, 8)] = fscale[0] * ((third - N3 / 2 + 0.5) * cell)

    def table_row(i, carry):
        angle = step_a * (splat(first_a) + i.astype(F32))
        tab_sa[pl.ds(pl.multiple_of(8 * i, 8), 8)] = fscale[2] * (0.5 * jnp.sin(angle))
        return carry

    lax.fori_loop(0, ROWS_A, table_row, 0)

    def table_ab(i, carry):
        row = lax.broadcasted_iota(jnp.int32, (8, 128), 0).astype(F32) + 8.0 * i.astype(F32)
        a = jnp.floor((row + 0.5) * (1.0 / COLS_B))
        b = row - a * COLS_B
        tab_ab[pl.ds(pl.multiple_of(8 * i, 8), 8)] = fscale[0] * (
            jnp.cos(step_a * (first_a + a)) - 0.5 * jnp.cos(step_b * (first_b + b))
        )
        return carry

    lax.fori_loop(0, 9, table_ab, 0)

    def table_lane(g, carry):
        last = g == GROUPS - 1
        piece = jnp.floor((lane8f + 0.5) * 0.0625)
        plane = jnp.where(last, piece, g.astype(F32))
        spot = jnp.where(last, 128.0 + lane8f - 16.0 * piece, lane8f)
        pair = jnp.floor((spot + 0.5) * 0.5)
        a = jnp.floor((pair + 0.5) * (1.0 / COLS_B))
        b = pair - a * COLS_B
        sin_b = jnp.sin(step_b * (first_b + b))
        x0 = (plane - PLANES / 2 + 0.5) * cell
        keep = plane < 4.0
        where = pl.ds(pl.multiple_of(8 * g, 8), 8)
        tab_l3[where] = jnp.where(keep, fscale[3] * (sin_b - x0), 0.0)
        tab_l4[where] = jnp.where(keep, fscale[4] * (jnp.cos(step_a * (first_a + a)) * sin_b), 0.0)
        return carry

    lax.fori_loop(0, GROUPS, table_lane, 0)
    locals_[0].wait()

    def start_side():
        remote(side_out, side_in, side_s, side_r, partner).start()

    def wait_side():
        remote(side_out, side_in, side_s, side_r, partner).wait_recv()

    def start_cols(a):
        at = pl.multiple_of(a * LINE, 8)
        to = pl.ds(pl.multiple_of(a * 72, 8), 72)
        remote(
            val.at[pl.ds(at + 72, 72)], ghost_bl.at[to], col_s.at[0], col_r.at[0, a], col_after
        ).start()
        remote(
            val.at[pl.ds(at, 72)], ghost_bh.at[to], col_s.at[1], col_r.at[1, a], col_before
        ).start()

    def lines_of(ref, first, b):
        return ref.reshape(ref.shape[0] // LINE, LINE, 128).at[
            pl.ds(first, 3), pl.ds(pl.multiple_of(b * CELL, 8), CELL)
        ]

    def start_edge(k):
        first, ghost, device = (
            (ROWS_A - 3, ghost_al, row_after), (0, ghost_ah, row_before)
        )[k]

        def body(b, carry):
            remote(
                lines_of(val, first, b), lines_of(ghost, 0, b),
                row_s.at[k], row_r.at[k, b], device,
            ).start()
            return carry

        lax.fori_loop(0, COLS_B, body, 0)

    def start_high():
        start_edge(0)

    def start_low():
        start_edge(1)

    def wait_rows(b):
        for k, ghost in enumerate((ghost_al, ghost_ah)):
            piece = lines_of(ghost, 0, b)
            remote(piece, piece, row_s.at[k], row_r.at[k, b], partner).wait_recv()

    def wait_cols(a):
        for k, ghost in enumerate((ghost_bl, ghost_bh)):
            piece = ghost.at[pl.ds(pl.multiple_of(a * 72, 8), 72)]
            remote(piece, piece, col_s.at[k], col_r.at[k, a], partner).wait_recv()

    def sent_halos():
        for k, ghost in enumerate((ghost_al, ghost_ah)):
            remote(ghost, ghost, row_s.at[k], row_r.at[k, 0], partner).wait_send()
        for k, ghost in enumerate((ghost_bl, ghost_bh)):
            remote(ghost, ghost, col_s.at[k], col_r.at[k, 0], partner).wait_send()
        remote(side_out, side_in, side_s, side_r, partner).wait_send()

    def tr_row(g, slot):
        return g * (SLOTS * PITCH) + slot * PITCH

    def to_transposed():
        def put(g, r, block):
            for k in range(16):
                merged = r * 128 + 8 * k
                row = tr_row(g, GHOST + merged // N4) + merged % N4
                tr[pl.ds(row, 8)] = block[8 * k:8 * k + 8]

        for g in range(GROUPS - 1):
            for r in range(3):
                put(g, r, val[pl.ds(r * PLANES + g, 128, stride=12)].T)
        for r in range(3):
            parts = [
                val[pl.ds(1536 + r * PLANES + p, 16, stride=12)] for p in range(PLANES)
            ]
            parts.append(jnp.zeros((64, 128), F32))
            put(GROUPS - 1, r, jnp.concatenate(parts, axis=0).T)

    is_low = half == 0
    turn = jnp.where(is_low, 127, 1)
    mine = jnp.where(is_low, lane8 & 1, 1 - (lane8 & 1)) == 0
    send_slot = jnp.where(is_low, GHOST + 5, GHOST)

    low_lanes = lane8 < 64
    SIDE = [(t, q) for t in range(3) for q in range(6)]

    def pack_side():
        def part(g, v):
            t, q = SIDE[v]
            return tr[pl.ds(tr_row(g, send_slot + t) + 8 * q, 8)]

        def pair(one, two):
            return jnp.where(mine, pltpu.roll(one, turn, 1), two)

        for k in range(2):
            for v in range(18):
                side_out[pl.ds(k * 144 + 8 * v, 8)] = pair(part(2 * k, v), part(2 * k + 1, v))
        for w in range(5):
            group = [part(4, min(4 * w + i, 17)) for i in range(4)]
            side_out[pl.ds(288 + 8 * w, 8)] = jnp.where(
                low_lanes, pair(group[0], group[1]), pltpu.roll(pair(group[2], group[3]), 64, 1)
            )

    def merge_side():
        back = jnp.where(is_low, 1, 127)
        for g in range(GROUPS):
            for v, (t, q) in enumerate(SIDE):
                at = 8 * q
                if g < 4:
                    got = side_in[pl.ds((g // 2) * 144 + 8 * v, 8)]
                    second = g % 2
                else:
                    got = side_in[pl.ds(288 + 8 * (v // 4), 8)]
                    second = v % 2
                    if v % 4 > 1:
                        got = pltpu.roll(got, 64, 1)
                    got = jnp.where(low_lanes, got, 0.0)
                if second:
                    got = pltpu.roll(got, back, 1)
                top = tr[pl.ds(tr_row(g, GHOST + 7) + at, 8)]
                bottom = tr[pl.ds(tr_row(g, GHOST) + at, 8)]
                up = pltpu.roll(tr[pl.ds(tr_row(g, GHOST + t) + at, 8)], 127, 1)
                down = pltpu.roll(tr[pl.ds(tr_row(g, GHOST + 5 + t) + at, 8)], 1, 1)
                tr[pl.ds(tr_row(g, GHOST + 8 + t) + at, 8)] = jnp.where(
                    odd, jnp.where(is_low, got, top), up
                )
                tr[pl.ds(tr_row(g, t) + at, 8)] = jnp.where(
                    odd, down, jnp.where(is_low, bottom, got)
                )

    def cell_out(left, right, flow, square, factor, peak):
        total = left + right
        gap = right - left
        rest = flow - total
        peak = jnp.maximum(peak, jnp.abs(rest) + jnp.abs(gap))
        return gap, (square - rest * rest) * factor, peak

    zero = jnp.zeros((8, 128), F32)

    def along_planes(first, end, peak):
        def body(n, peak):
            i, c = lax.div(n, CHUNKS), lax.rem(n, CHUNKS)
            q = jnp.where(i < 4, half * 5 + i, jnp.where(i == 4, 4, other * 5 + i - 5))
            start = q * (8 * CELL) + c * PLANES
            rows = [pl.ds(start + p, 8, stride=CELL) for p in range(PLANES)]
            got = [val[rows[p]] for p in range(PLANES)]
            flow = tab_ab[pl.ds(pl.multiple_of(8 * q, 8), 8)] + tab_x3[
                pl.ds(pl.multiple_of(8 * c, 8), 8)
            ]
            square = flow * flow
            line = [got[0]] * 3 + got + [got[3]] * 3
            for p, (left, right) in enumerate(chain(line)):
                left = zero if left is None else left
                right = zero if right is None else right
                gap, part, peak = cell_out(left, right, flow, square, kk[0], peak)
                d_p[rows[p]] = gap
                hn[rows[p]] = part
            return peak

        return lax.fori_loop(first * CHUNKS, end * CHUNKS, body, peak, unroll=2)

    def row_chain(n, peak):
        at = pl.multiple_of(8 * n, 8)
        line = (
            [ghost_al[pl.ds(i * LINE + at, 8)] for i in range(3)]
            + [val[pl.ds(a * LINE + at, 8)] for a in range(ROWS_A)]
            + [ghost_ah[pl.ds(i * LINE + at, 8)] for i in range(3)]
        )
        flow = tab_f1[pl.ds(pl.multiple_of(8 * lax.rem(n, 3), 8), 8)]
        square = flow * flow
        for a, (left, right) in enumerate(chain(line)):
            gap, part, peak = cell_out(left, right, flow, square, kk[1], peak)
            where = pl.ds(a * LINE + at, 8)
            d_a[where] = gap
            hn[where] += part
        return peak

    def col_chain(a, j, peak):
        ghost = pl.multiple_of(a * 72 + 8 * j, 8)
        at = pl.multiple_of(a * LINE + 8 * j, 8)
        line = (
            [ghost_bl[pl.ds(ghost + i * CELL, 8)] for i in range(3)]
            + [val[pl.ds(at + b * CELL, 8)] for b in range(COLS_B)]
            + [ghost_bh[pl.ds(ghost + i * CELL, 8)] for i in range(3)]
        )
        flow = tab_f2[pl.ds(pl.multiple_of(8 * j, 8), 8)] + tab_sa[
            pl.ds(pl.multiple_of(8 * a, 8), 8)
        ]
        square = flow * flow
        for b, (left, right) in enumerate(chain(line)):
            gap, part, peak = cell_out(left, right, flow, square, kk[2], peak)
            where = pl.ds(at + b * CELL, 8)
            d_b[where] = gap
            hn[where] += part
        return peak

    def along_edges():
        def body(k, peaks):
            row_peak, col_peak = peaks
            wait_rows(k)
            for j in range(3):
                row_peak = row_chain(3 * k + j, row_peak)
            for i in range(2):
                a = line_order(2 * k + i)
                wait_cols(a)
                for j in range(3):
                    col_peak = col_chain(a, j, col_peak)
            return row_peak, col_peak

        return lax.fori_loop(0, COLS_B, body, (zero, zero))

    def along_third():
        def body(n, peak):
            g, q = lax.div(n, 6), lax.rem(n, 6)
            line = [tr[pl.ds(tr_row(g, s) + 8 * q, 8)] for s in range(SLOTS)]
            flow = tab_l3[pl.ds(pl.multiple_of(8 * g, 8), 8)]
            square = flow * flow
            for s, (left, right) in enumerate(chain(line)):
                gap, part, peak = cell_out(left, right, flow, square, kk[3], peak)
                where = pl.ds((g * 8 + s) * PITCH + 8 * q, 8)
                d_3[where] = gap
                ht[where] += part
            return peak

        return lax.fori_loop(0, GROUPS * 6, body, zero, unroll=2)

    slope4 = fscale[4] * cell

    def along_fourth():
        def body(n, peak):
            g, seg = lax.div(n, 4), lax.rem(n, 4)
            first = seg * 12
            line = []
            for i in range(-3, 15):
                at = first + i
                if i < 0:
                    at = jnp.maximum(at, 0)
                if i > 11:
                    at = jnp.minimum(at, N4 - 1)
                line.append(tr[pl.ds(tr_row(g, GHOST) + at, 8, stride=PITCH)])
            table = tab_l4[pl.ds(pl.multiple_of(8 * g, 8), 8)]
            base = table - slope4 * (first.astype(F32) - (N4 / 2 - 0.5))
            for i, (left, right) in enumerate(chain(line)):
                flow = base - slope4 * float(i)
                gap, part, peak = cell_out(left, right, flow, flow * flow, kk[4], peak)
                where = pl.ds(g * 8 * PITCH + first + i, 8, stride=PITCH)
                d_4[where] = gap
                ht[where] = part
            return peak

        return lax.fori_loop(0, GROUPS * 4, body, zero, unroll=1)

    def greet(k):
        if k < len(ROUNDS):
            devices = [(lax.rem(gx + dx, 8), lax.rem(gy + dy, 16)) for dx, dy in ROUNDS[k]]
        else:
            devices = [partner]
        for device in devices:
            pl.semaphore_signal(met.at[k], inc=1, device_id=device, device_id_type=MESH)

    def met_all(k):
        pl.semaphore_wait(met.at[k], len(ROUNDS[k]) if k < len(ROUNDS) else 1)

    def speeds(step, peaks):
        row = jnp.zeros((1, 128), F32)
        lane = lax.broadcasted_iota(jnp.int32, (1, 128), 1)
        for i, peak in enumerate(peaks):
            row = jnp.where(lane == i, jnp.max(peak), row)
        ar_src[step] = row
        ar_buf[step, me] = row

        for dx, dy in FAR_FIRST:
            remote(
                ar_src.at[step], ar_buf.at[step, me], ar_s.at[step], ar_r.at[step],
                (lax.rem(gx + dx, 8), lax.rem(gy + dy, 16)),
            ).start()

    def all_speeds(step):
        every = ar_buf.at[step, pl.ds(0, 127)]
        whole_row = remote(every, every, ar_s.at[step], ar_r.at[step], partner)
        whole_row.wait_recv()
        best = jnp.max(ar_buf[step], axis=0)
        whole_row.wait_send()
        speed = []
        for i in range(5):
            lane_max = jnp.broadcast_to(best[:, i:i + 1], (8, 128))
            speed.append(lane_max * (costs[i] * (1.0 / 12.0)))
        summed = zero
        for i in range(5):
            summed = summed + speed[i] / SPACING[i]
        time_step = 0.5 / (summed + 1e-6)
        steps_out[step] = time_step[0, 0]
        return time_step, [
            time_step * speed[i] * (1.0 / (12.0 * SPACING[i])) for i in range(5)
        ]

    def from_transposed(dt, coef):
        def take(g, r):
            parts = []
            for k in range(16):
                merged = r * 128 + 8 * k
                row = (g * 8 + merged // N4) * PITCH + merged % N4
                where = pl.ds(row, 8)
                parts.append(coef[3] * d_3[where] + coef[4] * d_4[where] - dt * ht[where])
            return jnp.concatenate(parts, axis=0).T

        for g in range(GROUPS - 1):
            for r in range(3):
                wn[pl.ds(r * PLANES + g, 128, stride=12)] = take(g, r)
        for r in range(3):
            block = take(GROUPS - 1, r)
            for p in range(PLANES):
                wn[pl.ds(1536 + r * PLANES + p, 16, stride=12)] = block[16 * p:16 * p + 16]

    def new_line(a, dt, coef):
        for i in range(LINE // 8):
            where = pl.ds(pl.multiple_of(a * LINE + 8 * i, 8), 8)
            moved = val[where] + wn[where] - dt * hn[where]
            moved = moved + coef[0] * d_p[where] + coef[1] * d_a[where] + coef[2] * d_b[where]
            val[where] = jnp.maximum(jnp.minimum(moved, hi[where]), lo[where])

    def update(dt, coef):
        line_of = line_order

        def body(n, carry):
            new_line(line_of(n), dt, coef)

            @pl.when(n > 0)
            def _():
                start_cols(line_of(n - 1))

            @pl.when(n == 3)
            def _():
                start_low()

            @pl.when(n == 6)
            def _():
                start_high()

            return carry

        lax.fori_loop(0, ROWS_A, body, 0)
        start_cols(8)

    def last_update(dt, coef):
        def move(a, launch):
            launch(cells_of(val, a * COLS_B, COLS_B), pl.ds(lax.rem(a, 6) * COLS_B, COLS_B))

        mine_out = pl.ds(pl.multiple_of(half * CELL, 8), CELL)

        def far(src, to):
            remote(src, out_hbm.at[to, mine_out], out_s, out_r, partner).start()

        def near(src, to):
            pltpu.make_async_copy(src, out_hbm.at[to, mine_out], out_sem).start()

        for first, launch in ((other * 6, far), (half * 6, near)):
            def body(n, carry, first=first, launch=launch):
                new_line(first + n, dt, coef)

                @pl.when(n > 0)
                def _():
                    move(first + n - 1, launch)

                return carry

            lax.fori_loop(0, 6, body, 0)
            move(first + 5, launch)
        pltpu.make_async_copy(
            cells_of(val, half * 36, 36), part_of(out_hbm, half), out_sem
        ).wait()
        sent = remote(
            cells_of(val, other * 36, 36), part_of(out_hbm, other), out_s, out_r, partner
        )
        sent.wait_send()
        sent.wait_recv()

    def bounds(which):
        def body(n, carry):
            for i in range(9):
                where = pl.ds(pl.multiple_of(which * (TOTAL // 2) + 72 * n + 8 * i, 8), 8)
                hi[where] = jnp.where(mask_t[where] == 1, -0.5, BIG)
                lo[where] = jnp.where(mask_o[where] == 1, 0.5, -BIG)
            return carry

        lax.fori_loop(0, TOTAL // 144, body, 0)

    def own_cols(a, carry):
        start_cols(half * 6 + a)
        return carry

    def other_cols(a, carry):
        start_cols(other * 6 + a)
        return carry

    lax.fori_loop(0, 6, own_cols, 0)
    greet(0)
    early = along_planes(0, 4, zero)
    met_all(0)
    greet(1)
    swaps[0].wait_recv()
    lax.fori_loop(0, 6, other_cols, 0)
    start_low()
    start_high()

    for step in range(STEPS):
        to_transposed()
        pack_side()
        start_side()
        if step == 0:
            swaps[1].start()
            swaps[2].start()
            peak_p = along_planes(4, 9, early)
            met_all(1)
            greet(2)
        else:
            peak_p = along_planes(0, 9, zero)
        peak_4 = along_fourth()
        if step == 0:
            met_all(2)
            greet(3)
        peak_a, peak_b = along_edges()
        if step == 0:
            met_all(3)
            greet(4)
        wait_side()
        merge_side()
        if step == 0:
            met_all(4)
            greet(5)
        peak_3 = along_third()
        if step == 0:
            met_all(5)
        speeds(step, [peak_p, peak_a, peak_b, peak_3, peak_4])
        sent_halos()
        if step == 0:
            swaps[3].start()
            for k in (1, 2):
                locals_[k].wait()
            bounds(half)
        dt, coef = all_speeds(step)
        from_transposed(dt, coef)
        if step == 0:
            for k in (1, 2, 3):
                swaps[k].wait_recv()
            bounds(other)
            for k in range(4):
                swaps[k].wait_send()
        if step < STEPS - 1:
            update(dt, coef)
        else:
            last_update(dt, coef)


def to_rows(x):
    x = x.transpose(1, 2, 0, 3).reshape(6, 6, PLANES, 12, 128)
    x = with_layout_constraint(x, Layout((0, 1, 3, 2, 4)))
    return x.transpose(0, 1, 3, 2, 4).reshape(36, 48, 128)


def from_rows(x):
    x = x.reshape(6, 6, 12, PLANES, 128).transpose(0, 1, 3, 2, 4)
    return x.reshape(6, 6, PLANES, 1536).transpose(2, 0, 1, 3)


def solution(mesh):
    def rows(n):
        return pltpu.VMEM((n, 128), F32)

    dma = pltpu.SemaphoreType.DMA
    trans = GROUPS * 8 * PITCH
    scratch = [
        rows(TOTAL), rows(TOTAL), rows(TOTAL), rows(TOTAL), rows(TOTAL), rows(TOTAL),
        rows(TOTAL), rows(TOTAL),
        rows(3 * LINE), rows(3 * LINE), rows(ROWS_A * 72), rows(ROWS_A * 72),
        rows(GROUPS * SLOTS * PITCH), rows(trans), rows(trans), rows(trans),
        rows(328), rows(328),
        pltpu.VMEM((TOTAL, 128), jnp.int32), pltpu.VMEM((TOTAL, 128), jnp.int32),
        rows(24), rows(24), rows(8 * ROWS_A), rows(72), rows(8 * CHUNKS),
        rows(8 * GROUPS), rows(8 * GROUPS),
        pltpu.VMEM((STEPS, 1, 128), F32), pltpu.VMEM((STEPS, 128, 1, 128), F32),
        pltpu.SemaphoreType.REGULAR((6,)),
        dma((3,)), dma((4,)), dma((4,)),
        dma((2,)), dma((2, COLS_B)), dma((2,)), dma((2, ROWS_A)), dma(()), dma(()),
        dma((STEPS,)), dma((STEPS,)),
        dma(()), dma(()), dma(()),
    ]

    def body(value_field, target_mask, obstacle_mask, drift_gains, control_costs):
        anywhere = pl.BlockSpec(memory_space=pl.ANY)
        scalars = pl.BlockSpec(memory_space=pltpu.SMEM)
        moved, steps = pl.pallas_call(
            kernel,
            out_shape=(
                jax.ShapeDtypeStruct((36, 48, 128), F32),
                jax.ShapeDtypeStruct((STEPS,), F32),
            ),
            in_specs=[anywhere, anywhere, anywhere, scalars, scalars],
            out_specs=(anywhere, scalars),
            scratch_shapes=scratch,
            compiler_params=pltpu.CompilerParams(
                collective_id=0, has_side_effects=True, vmem_limit_bytes=53 * 2**20
            ),
        )(
            to_rows(value_field), to_rows(target_mask), to_rows(obstacle_mask),
            drift_gains, control_costs,
        )
        return from_rows(moved), steps

    grid = P(None, "gx", "gy", None)
    return jax.shard_map(
        body, mesh=mesh, in_specs=(grid, grid, grid, P(), P()), out_specs=(grid, P()),
        check_vma=False,
    )
```

```python
import functools
import math

import jax
import jax.numpy as jnp
from jax import lax
from jax.experimental import pallas as pl
from jax.experimental.pallas import tpu as pltpu
from jax.experimental.layout import Layout, with_layout_constraint
from jax.sharding import PartitionSpec as P

PLANES, N3, N4, GRID, STEPS, NA, NB = 4, 32, 48, 96, 3, 48, 96
SPACING = (2.0 / GRID, 2.0 * math.pi / NA, 2.0 * math.pi / NB, 2.0 / GRID, 2.0 / GRID)
MESH = pl.DeviceIdType.MESH
F32 = jnp.float32
BIG = 3.0e38

ROWS_A, COLS_B, CHUNKS = 12, 6, 6
CELL = PLANES * CHUNKS
LINE = COLS_B * CELL
TOTAL = ROWS_A * LINE
GROUPS = 5
PITCH = 52
SLOTS = 14
GHOST = 3
EPS = 0.75e-6
FIRST = 14
EARLY = 18


def _hops(offset):
    dx, dy = offset
    ring = lambda n: min(n, 4 - n)
    return ring(dx // 2) + 2 * (dx % 2) + ring(dy // 2 % 4) + dy // 8


FAR_FIRST = sorted(
    [(dx, dy) for dx in range(8) for dy in range(16) if dx or dy], key=_hops, reverse=True
)
ROUNDS = (((0, 1), (0, 15)), ((0, 2), (0, 14)), ((0, 4), (0, 12)), ((2, 0), (6, 0)), ((4, 0),))


def line_order(n):
    return jnp.where(n < 6, jnp.where(n < 3, n, n + 6), n - 3)


def _add(x, y):
    if x is None:
        return y
    if y is None:
        return x
    return x + y


def _sub(x, y):
    if y is None:
        return x
    if x is None:
        return -y
    return x - y


def _mul(x, y):
    if x is None or y is None:
        return None
    return x * y


def chain(values):
    cells = len(values) - 6
    diffs = [
        None if values[i] is values[i + 1] else values[i + 1] - values[i]
        for i in range(cells + 5)
    ]
    curve, twice, lean, weight_x, weight_y, weight_z = {}, {}, {}, {}, {}, {}
    previous = None

    def curve_at(i):
        if i not in curve:
            curve[i] = _sub(diffs[i + 1], diffs[i])
            twice[i] = _add(curve[i], curve[i])
            square = _mul(curve[i], curve[i])
            lean[i] = (square, _mul(square, 1.5))
        return curve[i]

    def smooth_at(i):
        if i not in weight_x:
            now, last = curve_at(i), curve_at(i - 1)
            cross = _mul(now, last)
            base = _add(lean[i][0], lean[i - 1][0])
            base = EPS if base is None else base + EPS
            middle = _sub(base, _mul(cross, 2.75))
            x = _add(middle, lean[i][1])
            y = _add(middle, lean[i - 1][1])
            z = _add(middle, _mul(cross, 1.5))
            weight_x[i], weight_y[i], weight_z[i] = x * x, y * y, z * z

    def third_at(i):
        return _sub(_add(curve_at(i + 1), curve_at(i - 1)), twice[i])

    thirds = {}
    for face in range(2, cells + 3):
        for i in (face - 1, face, face + 1):
            smooth_at(i)
        one, two, three = weight_x[face - 1], weight_z[face], weight_y[face + 1]
        w_low, w_mid, w_high = two * three, one * three, one * two
        for i in (face - 1, face):
            if i not in thirds:
                thirds[i] = third_at(i)
        low = _mul(thirds[face - 1], w_low)
        high = _mul(thirds[face], w_high)
        base = ((w_low + w_high) + (w_mid + w_mid)) * 1.5
        now, last = curve[face], curve[face - 1]
        scaled = _mul(diffs[face], 6.0)
        left = right = None
        if face < cells + 2:
            top = _add(low, _mul(high, 1.5))
            left = _add(scaled, _add(last, twice[face]))
            if top is not None:
                left = _sub(left, top * pl.reciprocal(base - w_low, approx=True))
        if face > 2:
            top = _add(_mul(low, 1.5), high)
            right = _sub(scaled, _add(now, twice[face - 1]))
            if top is not None:
                right = _add(right, top * pl.reciprocal(base - w_high, approx=True))
            yield previous, right
        previous = left


def kernel(
    value_hbm, target_hbm, obstacle_hbm, gains, costs,
    out_hbm, steps_out,
    val, hn, d_a, d_b, d_p, wn, hi, lo,
    ghost_al, ghost_ah, ghost_bl, ghost_bh,
    r_p, r_a, r_b, r_3, r_4, tab_f0,
    tr, ht, d_3, d_4, side_out, side_in,
    mask_t, mask_o,
    tab_f1, tab_f2, tab_sa, tab_ab, tab_x3, tab_l3, tab_l4,
    ar_src, ar_buf,
    met, local_sem, swap_s, swap_r, row_s, row_r, col_s, col_r, side_s, side_r, ar_s, ar_r, out_sem, out_s, out_r,
):
    gx, gy = lax.axis_index("gx"), lax.axis_index("gy")
    half = lax.rem(gx, 2)
    other = 1 - half
    partner = (gx + 1 - 2 * half, gy)
    me = gx * 16 + gy

    def remote(src, dst, send, recv, device):
        return pltpu.make_async_remote_copy(
            src_ref=src, dst_ref=dst, send_sem=send, recv_sem=recv,
            device_id=device, device_id_type=MESH,
        )

    row_before = (lax.rem(gx + 6, 8), gy)
    row_after = (lax.rem(gx + 2, 8), gy)
    col_before = (gx, lax.rem(gy + 15, 16))
    col_after = (gx, lax.rem(gy + 1, 16))
    barrier = pltpu.get_barrier_semaphore()
    for device in (partner, col_before, col_after, row_before, row_after):
        pl.semaphore_signal(barrier, inc=1, device_id=device, device_id_type=MESH)

    def part_of(ref, which):
        return ref.at[:, pl.ds(pl.multiple_of(which * CELL, 8), CELL)]

    inputs = (value_hbm, target_hbm, obstacle_hbm)
    places = (val, mask_t, mask_o)

    def cells_of(ref, first, count):
        return ref.reshape(TOTAL // CELL, CELL, 128).at[pl.ds(first, count)]

    def target_of(ref, first, count):
        return ref.at[pl.ds(first, count), pl.ds(pl.multiple_of(other * CELL, 8), CELL)]

    swaps = [
        remote(
            part_of(inputs[k], other), cells_of(places[k], half * 36, 36),
            swap_s.at[k], swap_r.at[k], partner,
        )
        for k in range(1)
    ]
    for k, (source, place, first, count) in enumerate((
        (target_hbm, mask_t, 0, FIRST), (target_hbm, mask_t, FIRST, 36 - FIRST),
        (obstacle_hbm, mask_o, 0, EARLY), (obstacle_hbm, mask_o, EARLY, 36 - EARLY),
    )):
        swaps.append(
            remote(
                target_of(source, first, count), cells_of(place, half * 36 + first, count),
                swap_s.at[1 + k], swap_r.at[1 + k], partner,
            )
        )
    locals_ = [
        pltpu.make_async_copy(
            part_of(inputs[k], half), cells_of(places[k], half * 36, 36), local_sem.at[k]
        )
        for k in range(3)
    ]
    for k in range(3):
        locals_[k].start()
    pl.semaphore_wait(barrier, 5)
    swaps[0].start()
    swaps[1].start()

    lane8 = lax.broadcasted_iota(jnp.int32, (8, 128), 1)
    lane8f = lane8.astype(F32)
    odd = (lane8 & 1) == 1

    def splat(scalar):
        return jnp.full((8, 128), scalar, F32)

    fscale = [splat(12.0 * gains[i]) / splat(costs[i]) for i in range(5)]
    kk = [costs[i] * (1.0 / (288.0 * SPACING[i])) for i in range(5)]
    half_f = half.astype(F32)
    first_a = (lax.div(gx, 2) * ROWS_A).astype(F32)
    first_b = (gy * COLS_B).astype(F32)
    step_a, step_b = 2.0 * math.pi / NA, 2.0 * math.pi / NB
    cell = 2.0 / GRID

    def split_lane(merged):
        third = jnp.floor((merged + 0.5) * (1.0 / N4))
        return third, merged - third * N4

    for block in range(3):
        row = lax.broadcasted_iota(jnp.int32, (8, 128), 0).astype(F32) + 8.0 * block
        chunk = jnp.floor((row + 0.5) * (1.0 / PLANES))
        plane = row - chunk * PLANES
        merged = (half_f * CHUNKS + chunk) * 128.0 + lane8f
        third, fourth = split_lane(merged)
        x0 = (plane - PLANES / 2 + 0.5) * cell
        x3 = (third - N3 / 2 + 0.5) * cell
        x4 = (fourth - N4 / 2 + 0.5) * cell
        tab_f1[pl.ds(8 * block, 8)] = fscale[1] * (x4 - 0.3 * x0)
        tab_f2[pl.ds(8 * block, 8)] = fscale[2] * x3
        tab_f0[pl.ds(8 * block, 8)] = fscale[0] * x3
    for chunk in range(CHUNKS):
        third, _ = split_lane((half_f * CHUNKS + chunk) * 128.0 + lane8f)
        tab_x3[pl.ds(8 * chunk, 8)] = fscale[0] * ((third - N3 / 2 + 0.5) * cell)

    def table_row(i, carry):
        angle = step_a * (splat(first_a) + i.astype(F32))
        tab_sa[pl.ds(pl.multiple_of(8 * i, 8), 8)] = fscale[2] * (0.5 * jnp.sin(angle))
        return carry

    lax.fori_loop(0, ROWS_A, table_row, 0)

    def table_ab(i, carry):
        row = lax.broadcasted_iota(jnp.int32, (8, 128), 0).astype(F32) + 8.0 * i.astype(F32)
        a = jnp.floor((row + 0.5) * (1.0 / COLS_B))
        b = row - a * COLS_B
        tab_ab[pl.ds(pl.multiple_of(8 * i, 8), 8)] = fscale[0] * (
            jnp.cos(step_a * (first_a + a)) - 0.5 * jnp.cos(step_b * (first_b + b))
        )
        return carry

    lax.fori_loop(0, 9, table_ab, 0)

    def table_lane(g, carry):
        last = g == GROUPS - 1
        piece = jnp.floor((lane8f + 0.5) * 0.0625)
        plane = jnp.where(last, piece, g.astype(F32))
        spot = jnp.where(last, 128.0 + lane8f - 16.0 * piece, lane8f)
        pair = jnp.floor((spot + 0.5) * 0.5)
        a = jnp.floor((pair + 0.5) * (1.0 / COLS_B))
        b = pair - a * COLS_B
        sin_b = jnp.sin(step_b * (first_b + b))
        x0 = (plane - PLANES / 2 + 0.5) * cell
        keep = plane < 4.0
        where = pl.ds(pl.multiple_of(8 * g, 8), 8)
        tab_l3[where] = jnp.where(keep, fscale[3] * (sin_b - x0), 0.0)
        tab_l4[where] = jnp.where(keep, fscale[4] * (jnp.cos(step_a * (first_a + a)) * sin_b), 0.0)
        return carry

    lax.fori_loop(0, GROUPS, table_lane, 0)
    locals_[0].wait()

    def start_side():
        remote(side_out, side_in, side_s, side_r, partner).start()

    def wait_side():
        remote(side_out, side_in, side_s, side_r, partner).wait_recv()

    def start_cols(a):
        at = pl.multiple_of(a * LINE, 8)
        to = pl.ds(pl.multiple_of(a * 72, 8), 72)
        remote(
            val.at[pl.ds(at + 72, 72)], ghost_bl.at[to], col_s.at[0], col_r.at[0, a], col_after
        ).start()
        remote(
            val.at[pl.ds(at, 72)], ghost_bh.at[to], col_s.at[1], col_r.at[1, a], col_before
        ).start()

    def lines_of(ref, first, b):
        return ref.reshape(ref.shape[0] // LINE, LINE, 128).at[
            pl.ds(first, 3), pl.ds(pl.multiple_of(b * CELL, 8), CELL)
        ]

    def start_edge(k):
        first, ghost, device = (
            (ROWS_A - 3, ghost_al, row_after), (0, ghost_ah, row_before)
        )[k]

        def body(b, carry):
            remote(
                lines_of(val, first, b), lines_of(ghost, 0, b),
                row_s.at[k], row_r.at[k, b], device,
            ).start()
            return carry

        lax.fori_loop(0, COLS_B, body, 0)

    def start_high():
        start_edge(0)

    def start_low():
        start_edge(1)

    def wait_rows(b):
        for k, ghost in enumerate((ghost_al, ghost_ah)):
            piece = lines_of(ghost, 0, b)
            remote(piece, piece, row_s.at[k], row_r.at[k, b], partner).wait_recv()

    def wait_cols(a):
        for k, ghost in enumerate((ghost_bl, ghost_bh)):
            piece = ghost.at[pl.ds(pl.multiple_of(a * 72, 8), 72)]
            remote(piece, piece, col_s.at[k], col_r.at[k, a], partner).wait_recv()

    def sent_halos():
        for k, ghost in enumerate((ghost_al, ghost_ah)):
            remote(ghost, ghost, row_s.at[k], row_r.at[k, 0], partner).wait_send()
        for k, ghost in enumerate((ghost_bl, ghost_bh)):
            remote(ghost, ghost, col_s.at[k], col_r.at[k, 0], partner).wait_send()
        remote(side_out, side_in, side_s, side_r, partner).wait_send()

    def tr_row(g, slot):
        return g * (SLOTS * PITCH) + slot * PITCH

    def to_transposed():
        def put(g, r, block):
            for k in range(16):
                merged = r * 128 + 8 * k
                row = tr_row(g, GHOST + merged // N4) + merged % N4
                tr[pl.ds(row, 8)] = block[8 * k:8 * k + 8]

        for g in range(GROUPS - 1):
            for r in range(3):
                put(g, r, val[pl.ds(r * PLANES + g, 128, stride=12)].T)
        for r in range(3):
            parts = [
                val[pl.ds(1536 + r * PLANES + p, 16, stride=12)] for p in range(PLANES)
            ]
            parts.append(jnp.zeros((64, 128), F32))
            put(GROUPS - 1, r, jnp.concatenate(parts, axis=0).T)

    is_low = half == 0
    turn = jnp.where(is_low, 127, 1)
    mine = jnp.where(is_low, lane8 & 1, 1 - (lane8 & 1)) == 0
    send_slot = jnp.where(is_low, GHOST + 5, GHOST)

    low_lanes = lane8 < 64
    SIDE = [(t, q) for t in range(3) for q in range(6)]

    def pack_side():
        def part(g, v):
            t, q = SIDE[v]
            return tr[pl.ds(tr_row(g, send_slot + t) + 8 * q, 8)]

        def pair(one, two):
            return jnp.where(mine, pltpu.roll(one, turn, 1), two)

        for k in range(2):
            for v in range(18):
                side_out[pl.ds(k * 144 + 8 * v, 8)] = pair(part(2 * k, v), part(2 * k + 1, v))
        for w in range(5):
            group = [part(4, min(4 * w + i, 17)) for i in range(4)]
            side_out[pl.ds(288 + 8 * w, 8)] = jnp.where(
                low_lanes, pair(group[0], group[1]), pltpu.roll(pair(group[2], group[3]), 64, 1)
            )

    def merge_side():
        back = jnp.where(is_low, 1, 127)
        for g in range(GROUPS):
            for v, (t, q) in enumerate(SIDE):
                at = 8 * q
                if g < 4:
                    got = side_in[pl.ds((g // 2) * 144 + 8 * v, 8)]
                    second = g % 2
                else:
                    got = side_in[pl.ds(288 + 8 * (v // 4), 8)]
                    second = v % 2
                    if v % 4 > 1:
                        got = pltpu.roll(got, 64, 1)
                    got = jnp.where(low_lanes, got, 0.0)
                if second:
                    got = pltpu.roll(got, back, 1)
                top = tr[pl.ds(tr_row(g, GHOST + 7) + at, 8)]
                bottom = tr[pl.ds(tr_row(g, GHOST) + at, 8)]
                up = pltpu.roll(tr[pl.ds(tr_row(g, GHOST + t) + at, 8)], 127, 1)
                down = pltpu.roll(tr[pl.ds(tr_row(g, GHOST + 5 + t) + at, 8)], 1, 1)
                tr[pl.ds(tr_row(g, GHOST + 8 + t) + at, 8)] = jnp.where(
                    odd, jnp.where(is_low, got, top), up
                )
                tr[pl.ds(tr_row(g, t) + at, 8)] = jnp.where(
                    odd, down, jnp.where(is_low, bottom, got)
                )

    def cell_out(left, right, flow, peak):
        gap = right - left
        rest = flow - (left + right)
        peak = jnp.maximum(peak, jnp.abs(rest) + jnp.abs(gap))
        return gap, rest, peak

    zero = jnp.zeros((8, 128), F32)

    def along_planes(first, end, peak):
        def body(n, peak):
            i, c = lax.div(n, CHUNKS), lax.rem(n, CHUNKS)
            q = jnp.where(i < 4, half * 5 + i, jnp.where(i == 4, 4, other * 5 + i - 5))
            start = q * (8 * CELL) + c * PLANES
            rows = [pl.ds(start + p, 8, stride=CELL) for p in range(PLANES)]
            got = [val[rows[p]] for p in range(PLANES)]
            flow = tab_ab[pl.ds(pl.multiple_of(8 * q, 8), 8)] + tab_x3[
                pl.ds(pl.multiple_of(8 * c, 8), 8)
            ]
            line = [got[0]] * 3 + got + [got[3]] * 3
            for p, (left, right) in enumerate(chain(line)):
                left = zero if left is None else left
                right = zero if right is None else right
                gap, rest, peak = cell_out(left, right, flow, peak)
                d_p[rows[p]] = gap
                r_p[rows[p]] = rest
            return peak

        return lax.fori_loop(first * CHUNKS, end * CHUNKS, body, peak, unroll=2)

    def row_chain(n, peak):
        at = pl.multiple_of(8 * n, 8)
        line = (
            [ghost_al[pl.ds(i * LINE + at, 8)] for i in range(3)]
            + [val[pl.ds(a * LINE + at, 8)] for a in range(ROWS_A)]
            + [ghost_ah[pl.ds(i * LINE + at, 8)] for i in range(3)]
        )
        flow = tab_f1[pl.ds(pl.multiple_of(8 * lax.rem(n, 3), 8), 8)]
        for a, (left, right) in enumerate(chain(line)):
            gap, rest, peak = cell_out(left, right, flow, peak)
            where = pl.ds(a * LINE + at, 8)
            d_a[where] = gap
            r_a[where] = rest
        return peak

    def col_chain(a, j, peak):
        ghost = pl.multiple_of(a * 72 + 8 * j, 8)
        at = pl.multiple_of(a * LINE + 8 * j, 8)
        line = (
            [ghost_bl[pl.ds(ghost + i * CELL, 8)] for i in range(3)]
            + [val[pl.ds(at + b * CELL, 8)] for b in range(COLS_B)]
            + [ghost_bh[pl.ds(ghost + i * CELL, 8)] for i in range(3)]
        )
        flow = tab_f2[pl.ds(pl.multiple_of(8 * j, 8), 8)] + tab_sa[
            pl.ds(pl.multiple_of(8 * a, 8), 8)
        ]
        for b, (left, right) in enumerate(chain(line)):
            gap, rest, peak = cell_out(left, right, flow, peak)
            where = pl.ds(at + b * CELL, 8)
            d_b[where] = gap
            r_b[where] = rest
        return peak

    def along_rows():
        def body(b, peak):
            wait_rows(b)
            for j in range(3):
                peak = row_chain(3 * b + j, peak)
            return peak

        return lax.fori_loop(0, COLS_B, body, zero)

    def along_cols(order):
        def body(k, peak):
            for i in range(2):
                a = order(2 * k + i)
                wait_cols(a)
                for j in range(3):
                    peak = col_chain(a, j, peak)
            return peak

        return lax.fori_loop(0, ROWS_A // 2, body, zero)

    def along_third():
        def body(n, peak):
            g, q = lax.div(n, 6), lax.rem(n, 6)
            line = [tr[pl.ds(tr_row(g, s) + 8 * q, 8)] for s in range(SLOTS)]
            flow = tab_l3[pl.ds(pl.multiple_of(8 * g, 8), 8)]
            for s, (left, right) in enumerate(chain(line)):
                gap, rest, peak = cell_out(left, right, flow, peak)
                where = pl.ds((g * 8 + s) * PITCH + 8 * q, 8)
                d_3[where] = gap
                r_3[where] = rest
            return peak

        return lax.fori_loop(0, GROUPS * 6, body, zero, unroll=2)

    slope4 = fscale[4] * cell

    def along_fourth():
        def body(n, peak):
            g, seg = lax.div(n, 4), lax.rem(n, 4)
            first = seg * 12
            line = []
            for i in range(-3, 15):
                at = first + i
                if i < 0:
                    at = jnp.maximum(at, 0)
                if i > 11:
                    at = jnp.minimum(at, N4 - 1)
                line.append(tr[pl.ds(tr_row(g, GHOST) + at, 8, stride=PITCH)])
            table = tab_l4[pl.ds(pl.multiple_of(8 * g, 8), 8)]
            base = table - slope4 * (first.astype(F32) - (N4 / 2 - 0.5))
            for i, (left, right) in enumerate(chain(line)):
                flow = base - slope4 * float(i)
                gap, rest, peak = cell_out(left, right, flow, peak)
                where = pl.ds(g * 8 * PITCH + first + i, 8, stride=PITCH)
                d_4[where] = gap
                r_4[where] = rest
            return peak

        return lax.fori_loop(0, GROUPS * 4, body, zero, unroll=1)

    def greet(k):
        if k < len(ROUNDS):
            devices = [(lax.rem(gx + dx, 8), lax.rem(gy + dy, 16)) for dx, dy in ROUNDS[k]]
        else:
            devices = [partner]
        for device in devices:
            pl.semaphore_signal(met.at[k], inc=1, device_id=device, device_id_type=MESH)

    def met_all(k):
        pl.semaphore_wait(met.at[k], len(ROUNDS[k]) if k < len(ROUNDS) else 1)

    def speeds(step, peaks):
        row = jnp.zeros((1, 128), F32)
        lane = lax.broadcasted_iota(jnp.int32, (1, 128), 1)
        for i, peak in enumerate(peaks):
            row = jnp.where(lane == i, jnp.max(peak), row)
        ar_src[step] = row
        ar_buf[step, me] = row

        for dx, dy in FAR_FIRST:
            remote(
                ar_src.at[step], ar_buf.at[step, me], ar_s.at[step], ar_r.at[step],
                (lax.rem(gx + dx, 8), lax.rem(gy + dy, 16)),
            ).start()

    def all_speeds(step):
        every = ar_buf.at[step, pl.ds(0, 127)]
        whole_row = remote(every, every, ar_s.at[step], ar_r.at[step], partner)
        whole_row.wait_recv()
        best = jnp.max(ar_buf[step], axis=0)
        whole_row.wait_send()
        speed = []
        for i in range(5):
            lane_max = jnp.broadcast_to(best[:, i:i + 1], (8, 128))
            speed.append(lane_max * (costs[i] * (1.0 / 12.0)))
        summed = zero
        for i in range(5):
            summed = summed + speed[i] / SPACING[i]
        time_step = 0.5 / (summed + 1e-6)
        steps_out[step] = time_step[0, 0]
        return time_step, [
            time_step * speed[i] * (1.0 / (12.0 * SPACING[i])) for i in range(5)
        ]

    def gather_terms():
        def natural(ab, carry):
            cos_part = tab_ab[pl.ds(ab, 8, stride=0)]
            sin_part = tab_sa[pl.ds(pl.multiple_of(8 * lax.div(ab, COLS_B), 8), 8)]
            for j in range(3):
                where = pl.ds(pl.multiple_of(ab * CELL + 8 * j, 8), 8)
                table = pl.ds(8 * j, 8)
                term = None
                for k, flow, rest in (
                    (0, tab_f0[table] + cos_part, r_p[where]),
                    (1, tab_f1[table], r_a[where]),
                    (2, tab_f2[table] + sin_part, r_b[where]),
                ):
                    part = (flow * flow - rest * rest) * kk[k]
                    term = part if term is None else term + part
                hn[where] = term
            return carry

        lax.fori_loop(0, TOTAL // CELL, natural, 0, unroll=2)
        eight = lax.broadcasted_iota(jnp.int32, (8, 128), 0).astype(F32)

        def turned(n, carry):
            g, s = lax.div(n, 8), lax.rem(n, 8)
            lanes = pl.ds(pl.multiple_of(8 * g, 8), 8)
            flow3 = tab_l3[lanes]
            base4 = tab_l4[lanes]
            square3 = flow3 * flow3
            for q in range(6):
                where = pl.ds((g * 8 + s) * PITCH + 8 * q, 8)
                flow4 = base4 - slope4 * (eight + (8.0 * q - (N4 / 2 - 0.5)))
                rest3, rest4 = r_3[where], r_4[where]
                ht[where] = (square3 - rest3 * rest3) * kk[3] + (
                    flow4 * flow4 - rest4 * rest4
                ) * kk[4]
            return carry

        lax.fori_loop(0, GROUPS * 8, turned, 0)

    def from_transposed(dt, coef):
        def take(g, r):
            parts = []
            for k in range(16):
                merged = r * 128 + 8 * k
                row = (g * 8 + merged // N4) * PITCH + merged % N4
                where = pl.ds(row, 8)
                parts.append(coef[3] * d_3[where] + coef[4] * d_4[where] - dt * ht[where])
            return jnp.concatenate(parts, axis=0).T

        for g in range(GROUPS - 1):
            for r in range(3):
                wn[pl.ds(r * PLANES + g, 128, stride=12)] = take(g, r)
        for r in range(3):
            block = take(GROUPS - 1, r)
            for p in range(PLANES):
                wn[pl.ds(1536 + r * PLANES + p, 16, stride=12)] = block[16 * p:16 * p + 16]

    def new_line(a, dt, coef):
        for i in range(LINE // 8):
            where = pl.ds(pl.multiple_of(a * LINE + 8 * i, 8), 8)
            moved = val[where] + wn[where] - dt * hn[where]
            moved = moved + coef[0] * d_p[where] + coef[1] * d_a[where] + coef[2] * d_b[where]
            val[where] = jnp.maximum(jnp.minimum(moved, hi[where]), lo[where])

    def update(dt, coef):
        line_of = line_order

        def body(n, carry):
            new_line(line_of(n), dt, coef)

            @pl.when(n == 3)
            def _():
                start_low()

            @pl.when(n == 6)
            def _():
                start_high()

            return carry

        lax.fori_loop(0, ROWS_A, body, 0)

    def last_update(dt, coef):
        def move(a, launch):
            launch(cells_of(val, a * COLS_B, COLS_B), pl.ds(lax.rem(a, 6) * COLS_B, COLS_B))

        mine_out = pl.ds(pl.multiple_of(half * CELL, 8), CELL)

        def far(src, to):
            remote(src, out_hbm.at[to, mine_out], out_s, out_r, partner).start()

        def near(src, to):
            pltpu.make_async_copy(src, out_hbm.at[to, mine_out], out_sem).start()

        for first, launch in ((other * 6, far), (half * 6, near)):
            def body(n, carry, first=first, launch=launch):
                new_line(first + n, dt, coef)

                @pl.when(n > 0)
                def _():
                    move(first + n - 1, launch)

                return carry

            lax.fori_loop(0, 6, body, 0)
            move(first + 5, launch)
        pltpu.make_async_copy(
            cells_of(val, half * 36, 36), part_of(out_hbm, half), out_sem
        ).wait()
        sent = remote(
            cells_of(val, other * 36, 36), part_of(out_hbm, other), out_s, out_r, partner
        )
        sent.wait_send()
        sent.wait_recv()

    def bounds(which):
        def body(n, carry):
            for i in range(9):
                where = pl.ds(pl.multiple_of(which * (TOTAL // 2) + 72 * n + 8 * i, 8), 8)
                hi[where] = jnp.where(mask_t[where] == 1, -0.5, BIG)
                lo[where] = jnp.where(mask_o[where] == 1, 0.5, -BIG)
            return carry

        lax.fori_loop(0, TOTAL // 144, body, 0)

    def own_cols(a, carry):
        start_cols(half * 6 + a)
        return carry

    def other_cols(a, carry):
        start_cols(other * 6 + a)
        return carry

    def all_cols(a, carry):
        start_cols(a)
        return carry

    def own_first(n):
        return jnp.where(n < 6, half * 6 + n, other * 6 + n - 6)

    lax.fori_loop(0, 6, own_cols, 0)
    greet(0)
    early = along_planes(0, 4, zero)
    met_all(0)
    greet(1)
    swaps[0].wait_recv()
    start_low()
    start_high()

    for step in range(STEPS):
        to_transposed()
        pack_side()
        start_side()
        if step == 0:
            lax.fori_loop(0, 6, other_cols, 0)
            swaps[2].start()
            swaps[3].start()
            peak_p = along_planes(4, 9, early)
            met_all(1)
            greet(2)
        else:
            lax.fori_loop(0, ROWS_A, all_cols, 0)
            peak_p = along_planes(0, 9, zero)
        peak_4 = along_fourth()
        if step == 0:
            met_all(2)
            greet(3)
        peak_a = along_rows()
        if step == 0:
            met_all(3)
            greet(4)
        wait_side()
        merge_side()
        peak_3 = along_third()
        if step == 0:
            met_all(4)
            greet(5)
        peak_b = along_cols(own_first if step == 0 else lambda n: n)
        if step == 0:
            met_all(5)
        speeds(step, [peak_p, peak_a, peak_b, peak_3, peak_4])
        gather_terms()
        sent_halos()
        if step == 0:
            swaps[4].start()
            for k in (1, 2):
                locals_[k].wait()
            bounds(half)
        dt, coef = all_speeds(step)
        from_transposed(dt, coef)
        if step == 0:
            for k in (1, 2, 3, 4):
                swaps[k].wait_recv()
            bounds(other)
            for k in range(5):
                swaps[k].wait_send()
        if step < STEPS - 1:
            update(dt, coef)
        else:
            last_update(dt, coef)


def to_rows(x):
    x = x.transpose(1, 2, 0, 3).reshape(6, 6, PLANES, 12, 128)
    x = with_layout_constraint(x, Layout((0, 1, 3, 2, 4)))
    return x.transpose(0, 1, 3, 2, 4).reshape(36, 48, 128)


def from_rows(x):
    x = x.reshape(6, 6, 12, PLANES, 128).transpose(0, 1, 3, 2, 4)
    return x.reshape(6, 6, PLANES, 1536).transpose(2, 0, 1, 3)


def solution(mesh):
    def rows(n):
        return pltpu.VMEM((n, 128), F32)

    dma = pltpu.SemaphoreType.DMA
    trans = GROUPS * 8 * PITCH
    scratch = [
        rows(TOTAL), rows(TOTAL), rows(TOTAL), rows(TOTAL), rows(TOTAL), rows(TOTAL),
        rows(TOTAL), rows(TOTAL),
        rows(3 * LINE), rows(3 * LINE), rows(ROWS_A * 72), rows(ROWS_A * 72),
        rows(TOTAL), rows(TOTAL), rows(TOTAL), rows(trans), rows(trans), rows(24),
        rows(GROUPS * SLOTS * PITCH), rows(trans), rows(trans), rows(trans),
        rows(328), rows(328),
        pltpu.VMEM((TOTAL, 128), jnp.int32), pltpu.VMEM((TOTAL, 128), jnp.int32),
        rows(24), rows(24), rows(8 * ROWS_A), rows(80), rows(8 * CHUNKS),
        rows(8 * GROUPS), rows(8 * GROUPS),
        pltpu.VMEM((STEPS, 1, 128), F32), pltpu.VMEM((STEPS, 128, 1, 128), F32),
        pltpu.SemaphoreType.REGULAR((6,)),
        dma((3,)), dma((5,)), dma((5,)),
        dma((2,)), dma((2, COLS_B)), dma((2,)), dma((2, ROWS_A)), dma(()), dma(()),
        dma((STEPS,)), dma((STEPS,)),
        dma(()), dma(()), dma(()),
    ]

    def body(value_field, target_mask, obstacle_mask, drift_gains, control_costs):
        anywhere = pl.BlockSpec(memory_space=pl.ANY)
        scalars = pl.BlockSpec(memory_space=pltpu.SMEM)
        moved, steps = pl.pallas_call(
            kernel,
            out_shape=(
                jax.ShapeDtypeStruct((36, 48, 128), F32),
                jax.ShapeDtypeStruct((STEPS,), F32),
            ),
            in_specs=[anywhere, anywhere, anywhere, scalars, scalars],
            out_specs=(anywhere, scalars),
            scratch_shapes=scratch,
            compiler_params=pltpu.CompilerParams(
                collective_id=0, has_side_effects=True, vmem_limit_bytes=53 * 2**20
            ),
        )(
            to_rows(value_field), to_rows(target_mask), to_rows(obstacle_mask),
            drift_gains, control_costs,
        )
        return from_rows(moved), steps

    grid = P(None, "gx", "gy", None)
    return jax.shard_map(
        body, mesh=mesh, in_specs=(grid, grid, grid, P(), P()), out_specs=(grid, P()),
        check_vma=False,
    )
```

```python
import functools
import math

import jax
import jax.numpy as jnp
from jax import lax
from jax.experimental import pallas as pl
from jax.experimental.pallas import tpu as pltpu
from jax.experimental.layout import Layout, with_layout_constraint
from jax.sharding import PartitionSpec as P

PLANES, N3, N4, GRID, STEPS, NA, NB = 4, 32, 48, 96, 3, 48, 96
SPACING = (2.0 / GRID, 2.0 * math.pi / NA, 2.0 * math.pi / NB, 2.0 / GRID, 2.0 / GRID)
MESH = pl.DeviceIdType.MESH
F32 = jnp.float32
BIG = 3.0e38

ROWS_A, COLS_B, CHUNKS = 12, 6, 6
CELL = PLANES * CHUNKS
LINE = COLS_B * CELL
TOTAL = ROWS_A * LINE
GROUPS = 5
PITCH = 52
SLOTS = 14
GHOST = 3
EPS = 0.75e-6
FIRST = 14
EARLY = 18


def _hops(offset):
    dx, dy = offset
    ring = lambda n: min(n, 4 - n)
    return ring(dx // 2) + 2 * (dx % 2) + ring(dy // 2 % 4) + dy // 8


FAR_FIRST = sorted(
    [(dx, dy) for dx in range(8) for dy in range(16) if dx or dy], key=_hops, reverse=True
)
ROUNDS = (((0, 1), (0, 15)), ((0, 2), (0, 14)), ((0, 4), (0, 12)), ((2, 0), (6, 0)), ((4, 0),))


def line_order(n):
    return jnp.where(n < 6, jnp.where(n < 3, n, n + 6), n - 3)


def _add(x, y):
    if x is None:
        return y
    if y is None:
        return x
    return x + y


def _sub(x, y):
    if y is None:
        return x
    if x is None:
        return -y
    return x - y


def _mul(x, y):
    if x is None or y is None:
        return None
    return x * y


def chain(values):
    cells = len(values) - 6
    diffs = [
        None if values[i] is values[i + 1] else values[i + 1] - values[i]
        for i in range(cells + 5)
    ]
    curve, twice, lean, weight_x, weight_y, weight_z = {}, {}, {}, {}, {}, {}
    previous = None

    def curve_at(i):
        if i not in curve:
            curve[i] = _sub(diffs[i + 1], diffs[i])
            twice[i] = _add(curve[i], curve[i])
            square = _mul(curve[i], curve[i])
            lean[i] = (square, _mul(square, 1.5))
        return curve[i]

    def smooth_at(i):
        if i not in weight_x:
            now, last = curve_at(i), curve_at(i - 1)
            cross = _mul(now, last)
            base = _add(lean[i][0], lean[i - 1][0])
            base = EPS if base is None else base + EPS
            middle = _sub(base, _mul(cross, 2.75))
            x = _add(middle, lean[i][1])
            y = _add(middle, lean[i - 1][1])
            z = _add(middle, _mul(cross, 1.5))
            weight_x[i], weight_y[i], weight_z[i] = x * x, y * y, z * z

    def third_at(i):
        return _sub(_add(curve_at(i + 1), curve_at(i - 1)), twice[i])

    thirds = {}
    for face in range(2, cells + 3):
        for i in (face - 1, face, face + 1):
            smooth_at(i)
        one, two, three = weight_x[face - 1], weight_z[face], weight_y[face + 1]
        w_low, w_mid, w_high = two * three, one * three, one * two
        for i in (face - 1, face):
            if i not in thirds:
                thirds[i] = third_at(i)
        low = _mul(thirds[face - 1], w_low)
        high = _mul(thirds[face], w_high)
        base = ((w_low + w_high) + (w_mid + w_mid)) * 1.5
        now, last = curve[face], curve[face - 1]
        scaled = _mul(diffs[face], 6.0)
        left = right = None
        if face < cells + 2:
            top = _add(low, _mul(high, 1.5))
            left = _add(scaled, _add(last, twice[face]))
            if top is not None:
                left = _sub(left, top * pl.reciprocal(base - w_low, approx=True))
        if face > 2:
            top = _add(_mul(low, 1.5), high)
            right = _sub(scaled, _add(now, twice[face - 1]))
            if top is not None:
                right = _add(right, top * pl.reciprocal(base - w_high, approx=True))
            yield previous, right
        previous = left


def kernel(
    value_hbm, target_hbm, obstacle_hbm, gains, costs,
    out_hbm, steps_out,
    val, hn, d_a, d_b, d_p, wn, hi, lo,
    ghost_al, ghost_ah, ghost_bl, ghost_bh,
    r_p, r_a, r_b, r_3, r_4, tab_f0,
    tr, ht, d_3, d_4, side_out, side_in,
    mask_t, mask_o,
    tab_f1, tab_f2, tab_sa, tab_ab, tab_x3, tab_l3, tab_l4,
    ar_src, ar_buf,
    met, local_sem, swap_s, swap_r, row_s, row_r, col_s, col_r, side_s, side_r, ar_s, ar_r, out_sem, out_s, out_r,
):
    gx, gy = lax.axis_index("gx"), lax.axis_index("gy")
    half = lax.rem(gx, 2)
    other = 1 - half
    partner = (gx + 1 - 2 * half, gy)
    me = gx * 16 + gy

    def remote(src, dst, send, recv, device):
        return pltpu.make_async_remote_copy(
            src_ref=src, dst_ref=dst, send_sem=send, recv_sem=recv,
            device_id=device, device_id_type=MESH,
        )

    row_before = (lax.rem(gx + 6, 8), gy)
    row_after = (lax.rem(gx + 2, 8), gy)
    col_before = (gx, lax.rem(gy + 15, 16))
    col_after = (gx, lax.rem(gy + 1, 16))
    barrier = pltpu.get_barrier_semaphore()
    for device in (partner, col_before, col_after, row_before, row_after):
        pl.semaphore_signal(barrier, inc=1, device_id=device, device_id_type=MESH)

    def part_of(ref, which):
        return ref.at[:, pl.ds(pl.multiple_of(which * CELL, 8), CELL)]

    inputs = (value_hbm, target_hbm, obstacle_hbm)
    places = (val, mask_t, mask_o)

    def cells_of(ref, first, count):
        return ref.reshape(TOTAL // CELL, CELL, 128).at[pl.ds(first, count)]

    def target_of(ref, first, count):
        return ref.at[pl.ds(first, count), pl.ds(pl.multiple_of(other * CELL, 8), CELL)]

    swaps = [
        remote(
            part_of(inputs[k], other), cells_of(places[k], half * 36, 36),
            swap_s.at[k], swap_r.at[k], partner,
        )
        for k in range(1)
    ]
    for k, (source, place, first, count) in enumerate((
        (target_hbm, mask_t, 0, FIRST), (target_hbm, mask_t, FIRST, 36 - FIRST),
        (obstacle_hbm, mask_o, 0, EARLY), (obstacle_hbm, mask_o, EARLY, 36 - EARLY),
    )):
        swaps.append(
            remote(
                target_of(source, first, count), cells_of(place, half * 36 + first, count),
                swap_s.at[1 + k], swap_r.at[1 + k], partner,
            )
        )
    locals_ = [
        pltpu.make_async_copy(
            part_of(inputs[k], half), cells_of(places[k], half * 36, 36), local_sem.at[k]
        )
        for k in range(3)
    ]
    for k in range(3):
        locals_[k].start()
    pl.semaphore_wait(barrier, 5)
    swaps[0].start()
    swaps[1].start()

    lane8 = lax.broadcasted_iota(jnp.int32, (8, 128), 1)
    lane8f = lane8.astype(F32)
    odd = (lane8 & 1) == 1

    def splat(scalar):
        return jnp.full((8, 128), scalar, F32)

    fscale = [splat(12.0 * gains[i]) / splat(costs[i]) for i in range(5)]
    kk = [costs[i] * (1.0 / (288.0 * SPACING[i])) for i in range(5)]
    half_f = half.astype(F32)
    first_a = (lax.div(gx, 2) * ROWS_A).astype(F32)
    first_b = (gy * COLS_B).astype(F32)
    step_a, step_b = 2.0 * math.pi / NA, 2.0 * math.pi / NB
    cell = 2.0 / GRID

    def split_lane(merged):
        third = jnp.floor((merged + 0.5) * (1.0 / N4))
        return third, merged - third * N4

    for block in range(3):
        row = lax.broadcasted_iota(jnp.int32, (8, 128), 0).astype(F32) + 8.0 * block
        chunk = jnp.floor((row + 0.5) * (1.0 / PLANES))
        plane = row - chunk * PLANES
        merged = (half_f * CHUNKS + chunk) * 128.0 + lane8f
        third, fourth = split_lane(merged)
        x0 = (plane - PLANES / 2 + 0.5) * cell
        x3 = (third - N3 / 2 + 0.5) * cell
        x4 = (fourth - N4 / 2 + 0.5) * cell
        tab_f1[pl.ds(8 * block, 8)] = fscale[1] * (x4 - 0.3 * x0)
        tab_f2[pl.ds(8 * block, 8)] = fscale[2] * x3
        tab_f0[pl.ds(8 * block, 8)] = fscale[0] * x3
    for chunk in range(CHUNKS):
        third, _ = split_lane((half_f * CHUNKS + chunk) * 128.0 + lane8f)
        tab_x3[pl.ds(8 * chunk, 8)] = fscale[0] * ((third - N3 / 2 + 0.5) * cell)

    def table_row(i, carry):
        angle = step_a * (splat(first_a) + i.astype(F32))
        tab_sa[pl.ds(pl.multiple_of(8 * i, 8), 8)] = fscale[2] * (0.5 * jnp.sin(angle))
        return carry

    lax.fori_loop(0, ROWS_A, table_row, 0)

    def table_ab(i, carry):
        row = lax.broadcasted_iota(jnp.int32, (8, 128), 0).astype(F32) + 8.0 * i.astype(F32)
        a = jnp.floor((row + 0.5) * (1.0 / COLS_B))
        b = row - a * COLS_B
        tab_ab[pl.ds(pl.multiple_of(8 * i, 8), 8)] = fscale[0] * (
            jnp.cos(step_a * (first_a + a)) - 0.5 * jnp.cos(step_b * (first_b + b))
        )
        return carry

    lax.fori_loop(0, 9, table_ab, 0)

    def table_lane(g, carry):
        last = g == GROUPS - 1
        piece = jnp.floor((lane8f + 0.5) * 0.0625)
        plane = jnp.where(last, piece, g.astype(F32))
        spot = jnp.where(last, 128.0 + lane8f - 16.0 * piece, lane8f)
        pair = jnp.floor((spot + 0.5) * 0.5)
        a = jnp.floor((pair + 0.5) * (1.0 / COLS_B))
        b = pair - a * COLS_B
        sin_b = jnp.sin(step_b * (first_b + b))
        x0 = (plane - PLANES / 2 + 0.5) * cell
        keep = plane < 4.0
        where = pl.ds(pl.multiple_of(8 * g, 8), 8)
        tab_l3[where] = jnp.where(keep, fscale[3] * (sin_b - x0), 0.0)
        tab_l4[where] = jnp.where(keep, fscale[4] * (jnp.cos(step_a * (first_a + a)) * sin_b), 0.0)
        return carry

    lax.fori_loop(0, GROUPS, table_lane, 0)
    locals_[0].wait()

    def start_side():
        remote(side_out, side_in, side_s, side_r, partner).start()

    def wait_side():
        remote(side_out, side_in, side_s, side_r, partner).wait_recv()

    def start_cols(a):
        at = pl.multiple_of(a * LINE, 8)
        to = pl.ds(pl.multiple_of(a * 72, 8), 72)
        remote(
            val.at[pl.ds(at + 72, 72)], ghost_bl.at[to], col_s.at[0], col_r.at[0, a], col_after
        ).start()
        remote(
            val.at[pl.ds(at, 72)], ghost_bh.at[to], col_s.at[1], col_r.at[1, a], col_before
        ).start()

    def lines_of(ref, first, b):
        return ref.reshape(ref.shape[0] // LINE, LINE, 128).at[
            pl.ds(first, 3), pl.ds(pl.multiple_of(b * CELL, 8), CELL)
        ]

    def start_edge(k):
        first, ghost, device = (
            (ROWS_A - 3, ghost_al, row_after), (0, ghost_ah, row_before)
        )[k]

        def body(b, carry):
            remote(
                lines_of(val, first, b), lines_of(ghost, 0, b),
                row_s.at[k], row_r.at[k, b], device,
            ).start()
            return carry

        lax.fori_loop(0, COLS_B, body, 0)

    def start_high():
        start_edge(0)

    def start_low():
        start_edge(1)

    def wait_rows(b):
        for k, ghost in enumerate((ghost_al, ghost_ah)):
            piece = lines_of(ghost, 0, b)
            remote(piece, piece, row_s.at[k], row_r.at[k, b], partner).wait_recv()

    def wait_cols(a):
        for k, ghost in enumerate((ghost_bl, ghost_bh)):
            piece = ghost.at[pl.ds(pl.multiple_of(a * 72, 8), 72)]
            remote(piece, piece, col_s.at[k], col_r.at[k, a], partner).wait_recv()

    def sent_halos():
        for k, ghost in enumerate((ghost_al, ghost_ah)):
            remote(ghost, ghost, row_s.at[k], row_r.at[k, 0], partner).wait_send()
        for k, ghost in enumerate((ghost_bl, ghost_bh)):
            remote(ghost, ghost, col_s.at[k], col_r.at[k, 0], partner).wait_send()
        remote(side_out, side_in, side_s, side_r, partner).wait_send()

    def tr_row(g, slot):
        return g * (SLOTS * PITCH) + slot * PITCH

    def to_transposed():
        def put(g, r, block):
            for k in range(16):
                merged = r * 128 + 8 * k
                row = tr_row(g, GHOST + merged // N4) + merged % N4
                tr[pl.ds(row, 8)] = block[8 * k:8 * k + 8]

        for g in range(GROUPS - 1):
            for r in range(3):
                put(g, r, val[pl.ds(r * PLANES + g, 128, stride=12)].T)
        for r in range(3):
            parts = [
                val[pl.ds(1536 + r * PLANES + p, 16, stride=12)] for p in range(PLANES)
            ]
            parts.append(jnp.zeros((64, 128), F32))
            put(GROUPS - 1, r, jnp.concatenate(parts, axis=0).T)

    is_low = half == 0
    turn = jnp.where(is_low, 127, 1)
    mine = jnp.where(is_low, lane8 & 1, 1 - (lane8 & 1)) == 0
    send_slot = jnp.where(is_low, GHOST + 5, GHOST)

    low_lanes = lane8 < 64
    SIDE = [(t, q) for t in range(3) for q in range(6)]

    def pack_side():
        def part(g, v):
            t, q = SIDE[v]
            return tr[pl.ds(tr_row(g, send_slot + t) + 8 * q, 8)]

        def pair(one, two):
            return jnp.where(mine, pltpu.roll(one, turn, 1), two)

        for k in range(2):
            for v in range(18):
                side_out[pl.ds(k * 144 + 8 * v, 8)] = pair(part(2 * k, v), part(2 * k + 1, v))
        for w in range(5):
            group = [part(4, min(4 * w + i, 17)) for i in range(4)]
            side_out[pl.ds(288 + 8 * w, 8)] = jnp.where(
                low_lanes, pair(group[0], group[1]), pltpu.roll(pair(group[2], group[3]), 64, 1)
            )

    def merge_side():
        back = jnp.where(is_low, 1, 127)
        for g in range(GROUPS):
            for v, (t, q) in enumerate(SIDE):
                at = 8 * q
                if g < 4:
                    got = side_in[pl.ds((g // 2) * 144 + 8 * v, 8)]
                    second = g % 2
                else:
                    got = side_in[pl.ds(288 + 8 * (v // 4), 8)]
                    second = v % 2
                    if v % 4 > 1:
                        got = pltpu.roll(got, 64, 1)
                    got = jnp.where(low_lanes, got, 0.0)
                if second:
                    got = pltpu.roll(got, back, 1)
                top = tr[pl.ds(tr_row(g, GHOST + 7) + at, 8)]
                bottom = tr[pl.ds(tr_row(g, GHOST) + at, 8)]
                up = pltpu.roll(tr[pl.ds(tr_row(g, GHOST + t) + at, 8)], 127, 1)
                down = pltpu.roll(tr[pl.ds(tr_row(g, GHOST + 5 + t) + at, 8)], 1, 1)
                tr[pl.ds(tr_row(g, GHOST + 8 + t) + at, 8)] = jnp.where(
                    odd, jnp.where(is_low, got, top), up
                )
                tr[pl.ds(tr_row(g, t) + at, 8)] = jnp.where(
                    odd, down, jnp.where(is_low, bottom, got)
                )

    def cell_out(left, right, flow, peak):
        gap = right - left
        rest = flow - (left + right)
        peak = jnp.maximum(peak, jnp.abs(rest) + jnp.abs(gap))
        return gap, rest, peak

    zero = jnp.zeros((8, 128), F32)

    def along_planes(first, end, peak):
        def body(n, peak):
            i, c = lax.div(n, CHUNKS), lax.rem(n, CHUNKS)
            q = jnp.where(i < 4, half * 5 + i, jnp.where(i == 4, 4, other * 5 + i - 5))
            start = q * (8 * CELL) + c * PLANES
            rows = [pl.ds(start + p, 8, stride=CELL) for p in range(PLANES)]
            got = [val[rows[p]] for p in range(PLANES)]
            flow = tab_ab[pl.ds(pl.multiple_of(8 * q, 8), 8)] + tab_x3[
                pl.ds(pl.multiple_of(8 * c, 8), 8)
            ]
            line = [got[0]] * 3 + got + [got[3]] * 3
            for p, (left, right) in enumerate(chain(line)):
                left = zero if left is None else left
                right = zero if right is None else right
                gap, rest, peak = cell_out(left, right, flow, peak)
                d_p[rows[p]] = gap
                r_p[rows[p]] = rest
            return peak

        return lax.fori_loop(first * CHUNKS, end * CHUNKS, body, peak, unroll=2)

    def row_chain(n, peak):
        at = pl.multiple_of(8 * n, 8)
        line = (
            [ghost_al[pl.ds(i * LINE + at, 8)] for i in range(3)]
            + [val[pl.ds(a * LINE + at, 8)] for a in range(ROWS_A)]
            + [ghost_ah[pl.ds(i * LINE + at, 8)] for i in range(3)]
        )
        flow = tab_f1[pl.ds(pl.multiple_of(8 * lax.rem(n, 3), 8), 8)]
        for a, (left, right) in enumerate(chain(line)):
            gap, rest, peak = cell_out(left, right, flow, peak)
            where = pl.ds(a * LINE + at, 8)
            d_a[where] = gap
            r_a[where] = rest
        return peak

    def col_chain(a, j, peak):
        ghost = pl.multiple_of(a * 72 + 8 * j, 8)
        at = pl.multiple_of(a * LINE + 8 * j, 8)
        line = (
            [ghost_bl[pl.ds(ghost + i * CELL, 8)] for i in range(3)]
            + [val[pl.ds(at + b * CELL, 8)] for b in range(COLS_B)]
            + [ghost_bh[pl.ds(ghost + i * CELL, 8)] for i in range(3)]
        )
        flow = tab_f2[pl.ds(pl.multiple_of(8 * j, 8), 8)] + tab_sa[
            pl.ds(pl.multiple_of(8 * a, 8), 8)
        ]
        for b, (left, right) in enumerate(chain(line)):
            gap, rest, peak = cell_out(left, right, flow, peak)
            where = pl.ds(at + b * CELL, 8)
            d_b[where] = gap
            r_b[where] = rest
        return peak

    def along_rows():
        def body(b, peak):
            wait_rows(b)
            for j in range(3):
                peak = row_chain(3 * b + j, peak)
            return peak

        return lax.fori_loop(0, COLS_B, body, zero)

    def along_cols(order):
        def body(k, peak):
            for i in range(2):
                a = order(2 * k + i)
                wait_cols(a)
                for j in range(3):
                    peak = col_chain(a, j, peak)
            return peak

        return lax.fori_loop(0, ROWS_A // 2, body, zero)

    def along_third():
        def body(n, peak):
            g, q = lax.div(n, 6), lax.rem(n, 6)
            line = [tr[pl.ds(tr_row(g, s) + 8 * q, 8)] for s in range(SLOTS)]
            flow = tab_l3[pl.ds(pl.multiple_of(8 * g, 8), 8)]
            for s, (left, right) in enumerate(chain(line)):
                gap, rest, peak = cell_out(left, right, flow, peak)
                where = pl.ds((g * 8 + s) * PITCH + 8 * q, 8)
                d_3[where] = gap
                r_3[where] = rest
            return peak

        return lax.fori_loop(0, GROUPS * 6, body, zero, unroll=2)

    slope4 = fscale[4] * cell

    def along_fourth():
        def body(n, peak):
            g, seg = lax.div(n, 4), lax.rem(n, 4)
            first = seg * 12
            line = []
            for i in range(-3, 15):
                at = first + i
                if i < 0:
                    at = jnp.maximum(at, 0)
                if i > 11:
                    at = jnp.minimum(at, N4 - 1)
                line.append(tr[pl.ds(tr_row(g, GHOST) + at, 8, stride=PITCH)])
            table = tab_l4[pl.ds(pl.multiple_of(8 * g, 8), 8)]
            base = table - slope4 * (first.astype(F32) - (N4 / 2 - 0.5))
            for i, (left, right) in enumerate(chain(line)):
                flow = base - slope4 * float(i)
                gap, rest, peak = cell_out(left, right, flow, peak)
                where = pl.ds(g * 8 * PITCH + first + i, 8, stride=PITCH)
                d_4[where] = gap
                r_4[where] = rest
            return peak

        return lax.fori_loop(0, GROUPS * 4, body, zero, unroll=1)

    def greet(k):
        if k < len(ROUNDS):
            devices = [(lax.rem(gx + dx, 8), lax.rem(gy + dy, 16)) for dx, dy in ROUNDS[k]]
        else:
            devices = [partner]
        for device in devices:
            pl.semaphore_signal(met.at[k], inc=1, device_id=device, device_id_type=MESH)

    def met_all(k):
        pl.semaphore_wait(met.at[k], len(ROUNDS[k]) if k < len(ROUNDS) else 1)

    def speeds(step, peaks):
        row = jnp.zeros((1, 128), F32)
        lane = lax.broadcasted_iota(jnp.int32, (1, 128), 1)
        for i, peak in enumerate(peaks):
            row = jnp.where(lane == i, jnp.max(peak), row)
        ar_src[step] = row
        ar_buf[step, me] = row

        for dx, dy in FAR_FIRST:
            remote(
                ar_src.at[step], ar_buf.at[step, me], ar_s.at[step], ar_r.at[step],
                (lax.rem(gx + dx, 8), lax.rem(gy + dy, 16)),
            ).start()

    def all_speeds(step):
        every = ar_buf.at[step, pl.ds(0, 127)]
        whole_row = remote(every, every, ar_s.at[step], ar_r.at[step], partner)
        whole_row.wait_recv()
        best = jnp.max(ar_buf[step], axis=0)
        whole_row.wait_send()
        speed = []
        for i in range(5):
            lane_max = jnp.broadcast_to(best[:, i:i + 1], (8, 128))
            speed.append(lane_max * (costs[i] * (1.0 / 12.0)))
        summed = zero
        for i in range(5):
            summed = summed + speed[i] / SPACING[i]
        time_step = 0.5 / (summed + 1e-6)
        steps_out[step] = time_step[0, 0]
        return time_step, [
            time_step * speed[i] * (1.0 / (12.0 * SPACING[i])) for i in range(5)
        ]

    def gather_terms():
        def natural(ab, carry):
            cos_part = tab_ab[pl.ds(ab, 8, stride=0)]
            sin_part = tab_sa[pl.ds(pl.multiple_of(8 * lax.div(ab, COLS_B), 8), 8)]
            for j in range(3):
                where = pl.ds(pl.multiple_of(ab * CELL + 8 * j, 8), 8)
                table = pl.ds(8 * j, 8)
                term = None
                for k, flow, rest in (
                    (0, tab_f0[table] + cos_part, r_p[where]),
                    (1, tab_f1[table], r_a[where]),
                    (2, tab_f2[table] + sin_part, r_b[where]),
                ):
                    part = (flow * flow - rest * rest) * kk[k]
                    term = part if term is None else term + part
                hn[where] = term
            return carry

        lax.fori_loop(0, TOTAL // CELL, natural, 0, unroll=2)
        eight = lax.broadcasted_iota(jnp.int32, (8, 128), 0).astype(F32)

        def turned(n, carry):
            g, s = lax.div(n, 8), lax.rem(n, 8)
            lanes = pl.ds(pl.multiple_of(8 * g, 8), 8)
            flow3 = tab_l3[lanes]
            base4 = tab_l4[lanes]
            square3 = flow3 * flow3
            for q in range(6):
                where = pl.ds((g * 8 + s) * PITCH + 8 * q, 8)
                flow4 = base4 - slope4 * (eight + (8.0 * q - (N4 / 2 - 0.5)))
                rest3, rest4 = r_3[where], r_4[where]
                ht[where] = (square3 - rest3 * rest3) * kk[3] + (
                    flow4 * flow4 - rest4 * rest4
                ) * kk[4]
            return carry

        lax.fori_loop(0, GROUPS * 8, turned, 0)

    def from_transposed(dt, coef):
        def take(g, r):
            parts = []
            for k in range(16):
                merged = r * 128 + 8 * k
                row = (g * 8 + merged // N4) * PITCH + merged % N4
                where = pl.ds(row, 8)
                parts.append(coef[3] * d_3[where] + coef[4] * d_4[where] - dt * ht[where])
            return jnp.concatenate(parts, axis=0).T

        for g in range(GROUPS - 1):
            for r in range(3):
                wn[pl.ds(r * PLANES + g, 128, stride=12)] = take(g, r)
        for r in range(3):
            block = take(GROUPS - 1, r)
            for p in range(PLANES):
                wn[pl.ds(1536 + r * PLANES + p, 16, stride=12)] = block[16 * p:16 * p + 16]

    def new_line(a, dt, coef):
        for i in range(LINE // 8):
            where = pl.ds(pl.multiple_of(a * LINE + 8 * i, 8), 8)
            moved = val[where] + wn[where] - dt * hn[where]
            moved = moved + coef[0] * d_p[where] + coef[1] * d_a[where] + coef[2] * d_b[where]
            val[where] = jnp.maximum(jnp.minimum(moved, hi[where]), lo[where])

    def update(dt, coef):
        line_of = line_order

        def body(n, carry):
            new_line(line_of(n), dt, coef)

            @pl.when(n == 3)
            def _():
                start_low()

            @pl.when(n == 6)
            def _():
                start_high()

            return carry

        lax.fori_loop(0, ROWS_A, body, 0)

    def last_update(dt, coef):
        def move(a, launch):
            launch(cells_of(val, a * COLS_B, COLS_B), pl.ds(lax.rem(a, 6) * COLS_B, COLS_B))

        mine_out = pl.ds(pl.multiple_of(half * CELL, 8), CELL)

        def far(src, to):
            remote(src, out_hbm.at[to, mine_out], out_s, out_r, partner).start()

        def near(src, to):
            pltpu.make_async_copy(src, out_hbm.at[to, mine_out], out_sem).start()

        for first, launch in ((other * 6, far), (half * 6, near)):
            def body(n, carry, first=first, launch=launch):
                new_line(first + n, dt, coef)

                @pl.when(n > 0)
                def _():
                    move(first + n - 1, launch)

                return carry

            lax.fori_loop(0, 6, body, 0)
            move(first + 5, launch)
        pltpu.make_async_copy(
            cells_of(val, half * 36, 36), part_of(out_hbm, half), out_sem
        ).wait()
        sent = remote(
            cells_of(val, other * 36, 36), part_of(out_hbm, other), out_s, out_r, partner
        )
        sent.wait_send()
        sent.wait_recv()

    def bounds(which):
        def body(n, carry):
            for i in range(9):
                where = pl.ds(pl.multiple_of(which * (TOTAL // 2) + 72 * n + 8 * i, 8), 8)
                hi[where] = jnp.where(mask_t[where] == 1, -0.5, BIG)
                lo[where] = jnp.where(mask_o[where] == 1, 0.5, -BIG)
            return carry

        lax.fori_loop(0, TOTAL // 144, body, 0)

    def own_cols(a, carry):
        start_cols(half * 6 + a)
        return carry

    def other_cols(a, carry):
        start_cols(other * 6 + a)
        return carry

    def all_cols(a, carry):
        start_cols(a)
        return carry

    def own_first(n):
        return jnp.where(n < 6, half * 6 + n, other * 6 + n - 6)

    greet(0)
    early = along_planes(0, 4, zero)
    met_all(0)
    greet(1)
    swaps[0].wait_recv()
    start_low()
    start_high()

    for step in range(STEPS):
        to_transposed()
        pack_side()
        start_side()
        if step == 0:
            lax.fori_loop(0, 6, own_cols, 0)
            lax.fori_loop(0, 6, other_cols, 0)
            swaps[2].start()
            swaps[3].start()
            peak_p = along_planes(4, 9, early)
            met_all(1)
            greet(2)
        else:
            lax.fori_loop(0, ROWS_A, all_cols, 0)
            peak_p = along_planes(0, 9, zero)
        peak_4 = along_fourth()
        if step == 0:
            met_all(2)
            greet(3)
        peak_a = along_rows()
        if step == 0:
            met_all(3)
            greet(4)
        wait_side()
        merge_side()
        peak_3 = along_third()
        if step == 0:
            met_all(4)
            greet(5)
        peak_b = along_cols(own_first if step == 0 else lambda n: n)
        if step == 0:
            met_all(5)
        speeds(step, [peak_p, peak_a, peak_b, peak_3, peak_4])
        gather_terms()
        sent_halos()
        if step == 0:
            swaps[4].start()
            for k in (1, 2):
                locals_[k].wait()
            bounds(half)
        dt, coef = all_speeds(step)
        from_transposed(dt, coef)
        if step == 0:
            for k in (1, 2, 3, 4):
                swaps[k].wait_recv()
            bounds(other)
            for k in range(5):
                swaps[k].wait_send()
        if step < STEPS - 1:
            update(dt, coef)
        else:
            last_update(dt, coef)


def to_rows(x):
    x = x.transpose(1, 2, 0, 3).reshape(6, 6, PLANES, 12, 128)
    x = with_layout_constraint(x, Layout((0, 1, 3, 2, 4)))
    return x.transpose(0, 1, 3, 2, 4).reshape(36, 48, 128)


def from_rows(x):
    x = x.reshape(6, 6, 12, PLANES, 128).transpose(0, 1, 3, 2, 4)
    return x.reshape(6, 6, PLANES, 1536).transpose(2, 0, 1, 3)


def solution(mesh):
    def rows(n):
        return pltpu.VMEM((n, 128), F32)

    dma = pltpu.SemaphoreType.DMA
    trans = GROUPS * 8 * PITCH
    scratch = [
        rows(TOTAL), rows(TOTAL), rows(TOTAL), rows(TOTAL), rows(TOTAL), rows(TOTAL),
        rows(TOTAL), rows(TOTAL),
        rows(3 * LINE), rows(3 * LINE), rows(ROWS_A * 72), rows(ROWS_A * 72),
        rows(TOTAL), rows(TOTAL), rows(TOTAL), rows(trans), rows(trans), rows(24),
        rows(GROUPS * SLOTS * PITCH), rows(trans), rows(trans), rows(trans),
        rows(328), rows(328),
        pltpu.VMEM((TOTAL, 128), jnp.int32), pltpu.VMEM((TOTAL, 128), jnp.int32),
        rows(24), rows(24), rows(8 * ROWS_A), rows(80), rows(8 * CHUNKS),
        rows(8 * GROUPS), rows(8 * GROUPS),
        pltpu.VMEM((STEPS, 1, 128), F32), pltpu.VMEM((STEPS, 128, 1, 128), F32),
        pltpu.SemaphoreType.REGULAR((6,)),
        dma((3,)), dma((5,)), dma((5,)),
        dma((2,)), dma((2, COLS_B)), dma((2,)), dma((2, ROWS_A)), dma(()), dma(()),
        dma((STEPS,)), dma((STEPS,)),
        dma(()), dma(()), dma(()),
    ]

    def body(value_field, target_mask, obstacle_mask, drift_gains, control_costs):
        anywhere = pl.BlockSpec(memory_space=pl.ANY)
        scalars = pl.BlockSpec(memory_space=pltpu.SMEM)
        moved, steps = pl.pallas_call(
            kernel,
            out_shape=(
                jax.ShapeDtypeStruct((36, 48, 128), F32),
                jax.ShapeDtypeStruct((STEPS,), F32),
            ),
            in_specs=[anywhere, anywhere, anywhere, scalars, scalars],
            out_specs=(anywhere, scalars),
            scratch_shapes=scratch,
            compiler_params=pltpu.CompilerParams(
                collective_id=0, has_side_effects=True, vmem_limit_bytes=53 * 2**20
            ),
        )(
            to_rows(value_field), to_rows(target_mask), to_rows(obstacle_mask),
            drift_gains, control_costs,
        )
        return from_rows(moved), steps

    grid = P(None, "gx", "gy", None)
    return jax.shard_map(
        body, mesh=mesh, in_specs=(grid, grid, grid, P(), P()), out_specs=(grid, P()),
        check_vma=False,
    )
```
